512 devices in a mesh: gx: 16 (over y, core), gy: 32 (over x, z).
Axes of the slice: x: 4, y: 8, z: 8, core: 2. Of those that a mesh axis runs over, the one named last changes fastest.
Arguments:
- incident: float32 [64, 512, 240], P('gx', 'gy'), may hold values from -13 to 13
- sphere_kinds: int32 [64, 512], P('gx', 'gy'), may hold values from 0 to 3
- pair_codes: int32 [64, 512, 64], P('gx', 'gy'), may hold values from 0 to 80
- operators: int32 [64, 512, 64], P('gx', 'gy'), may hold values from 0 to 23
- pair_valid: int32 [64, 512, 64], P('gx', 'gy'), may hold values 0 or 1
- translations: bfloat16 [24, 240, 240], replicated, may hold values from -0.03125 to 0.03125
- tmatrices: float32 [4, 240, 240], replicated, may hold values from -0.375 to 0.375
Outputs:
- solution: float32 [64, 512, 240], P('gx', 'gy')
- residual: float32 [64, 512, 240], P('gx', 'gy')
The draws below stay inside these ranges and needn't reach their ends.
All inputs are finite; a program needn't handle non-finite values. No bound on the sum of `pair_valid` on one device may be relied on, other than what follows from the above.
Results may differ from the reference program's by a relative error of at most 0.0038.
Values sent between devices are 32-bit elements; how exact they have to be, the bound alone decides.
A program may use at most 64 MiB of HBM per device.

```python
import jax
import jax.numpy as jnp
from jax import lax

C = 240
SLOTS = 64
HALO = 4
OPS = 24
KINDS = 4
NX = 64
NY = 512


def draw_incident(key, part):
    keys = jax.random.split(jax.random.fold_in(key, 17), 3)
    pos_x = jnp.arange(NX, dtype=jnp.float32)[:, None, None] / NX
    pos_y = jnp.arange(NY, dtype=jnp.float32)[None, :, None] / NY
    row_scale = jax.random.uniform(keys[1], (NX, NY, 1), jnp.float32, 0.0, 0.5)
    col_scale = jax.random.uniform(keys[2], (1, 1, C), jnp.float32, 0.0, 0.5)
    scale = 10.0 ** (0.5 * (pos_x + pos_y) + row_scale + col_scale - 1.5)
    values = jnp.clip(jax.random.normal(keys[0], (NX, NY, C), jnp.float32), -4.0, 4.0)
    return values * scale


def plant(entries, key, smallest, high):
    longest = entries.shape.index(max(entries.shape))
    spots = []
    for shift in (0, 1):
        where = [jax.random.randint(jax.random.fold_in(key, axis), (), 0, length) for axis, length in enumerate(entries.shape)]
        where[longest] = (where[longest] + shift) % entries.shape[longest]
        spots.append(tuple(where))
    return entries.at[spots[0]].set(smallest).at[spots[1]].set(high)


def scatter_about(stream_key, dims, deviation, most, kind=jnp.bfloat16):
    return jnp.clip(deviation * jax.random.normal(stream_key, dims, jnp.float32), -most, most).astype(kind)


def setup_inputs(seed: int = 0) -> dict:
    streams_of = jax.random.split(jax.random.key(seed), 8)
    incident = draw_incident(jax.random.fold_in(streams_of[7], 71), 0)
    sphere_kinds = plant(jax.random.randint(streams_of[1], (NX, NY), 0, KINDS), jax.random.fold_in(streams_of[1], 1), 0, KINDS - 1).astype(jnp.int32)
    pair_codes = plant(jax.random.randint(streams_of[2], (NX, NY, SLOTS), 0, (2 * HALO + 1) ** 2), jax.random.fold_in(streams_of[2], 1), 0, ((2 * HALO + 1) ** 2) - 1).astype(jnp.int32)
    operators = plant(jax.random.randint(streams_of[3], (NX, NY, SLOTS), 0, OPS), jax.random.fold_in(streams_of[3], 1), 0, OPS - 1).astype(jnp.int32)
    pair_valid = plant((jax.random.randint(streams_of[4], (NX, NY, SLOTS), 0, 2) < 1).astype(jnp.int32), jax.random.fold_in(streams_of[4], 1), 0, 1)
    translations = scatter_about(streams_of[5], (OPS, C, C), (2 * C * SLOTS) ** -0.5, 0.03125)
    tmatrices = scatter_about(streams_of[6], (KINDS, C, C), C ** -0.5, 0.375, jnp.float32)
    return dict(incident=incident, sphere_kinds=sphere_kinds, pair_codes=pair_codes, operators=operators, pair_valid=pair_valid, translations=translations, tmatrices=tmatrices)


epsilon = 1e-06

def kind_row(tmatrices, kinds_row, values_row):
    selector = (kinds_row[:, None] == jnp.arange(tmatrices.shape[0], dtype=jnp.int32)[None, :]).astype(jnp.float32)
    per_kind = jnp.einsum('pcd,id->pic', tmatrices, values_row, precision=lax.Precision.HIGHEST)
    return jnp.einsum('ip,pic->ic', selector, per_kind, precision=lax.Precision.HIGHEST)

def apply_kinds(values, sphere_kinds, tmatrices):

    def one_row(index):
        kinds_row = lax.dynamic_index_in_dim(sphere_kinds, index, 0, keepdims=False)
        values_row = lax.dynamic_index_in_dim(values, index, 0, keepdims=False)
        return kind_row(tmatrices, kinds_row, values_row)
    return lax.map(one_row, jnp.arange(NX, dtype=jnp.int32))

def operate(values, sphere_kinds, pair_codes, operators, pair_valid, translations, tmatrices):
    extended = jnp.pad(values, ((HALO, HALO), (HALO, HALO), (0, 0)))
    stride = 2 * HALO + 1
    line_width = NY + 2 * HALO
    count_ops = translations.shape[0]
    trans_wide = translations.astype(jnp.float32)
    zero_index = jnp.zeros((), jnp.int32)

    def one_row(index):
        window = lax.dynamic_slice(extended, (index, zero_index, zero_index), (stride, line_width, C))
        flattened = window.reshape(stride * line_width, C)
        codes_row = lax.dynamic_index_in_dim(pair_codes, index, 0, keepdims=False)
        ops_row = lax.dynamic_index_in_dim(operators, index, 0, keepdims=False)
        valid_row = lax.dynamic_index_in_dim(pair_valid, index, 0, keepdims=False)
        column = jnp.arange(NY, dtype=jnp.int32)[:, None]
        targets = codes_row // stride * line_width + column + codes_row % stride
        picked = jnp.take(flattened, targets, axis=0)
        chosen = (ops_row[..., None] == jnp.arange(count_ops, dtype=jnp.int32)).astype(jnp.float32) * valid_row[..., None].astype(jnp.float32)
        grouped = jnp.einsum('isk,isc->kic', chosen, picked, precision=lax.Precision.HIGHEST)
        grouped = lax.optimization_barrier(grouped.astype(jnp.bfloat16)).astype(jnp.float32)
        moved = jnp.einsum('kcd,kid->ic', trans_wide, grouped, precision=lax.Precision.HIGHEST)
        kinds_row = lax.dynamic_index_in_dim(sphere_kinds, index, 0, keepdims=False)
        values_row = lax.dynamic_index_in_dim(values, index, 0, keepdims=False)
        return values_row - kind_row(tmatrices, kinds_row, moved)
    return lax.map(one_row, jnp.arange(NX, dtype=jnp.int32))

def reference(incident, sphere_kinds, pair_codes, operators, pair_valid, translations, tmatrices):

    def apply_op(values):
        return operate(values, sphere_kinds, pair_codes, operators, pair_valid, translations, tmatrices)
    source = apply_kinds(incident, sphere_kinds, tmatrices)
    beta = jnp.sqrt(jnp.sum(source * source) + epsilon)
    first = source / beta
    image_one = apply_op(first)
    h_one_one = jnp.sum(image_one * first)
    rest = image_one - h_one_one * first
    h_two_one = jnp.sqrt(jnp.sum(rest * rest) + epsilon)
    second = rest / h_two_one
    image_two = apply_op(second)
    h_one_two = jnp.sum(image_two * first)
    rest = image_two - h_one_two * first
    h_two_two = jnp.sum(rest * second)
    rest = rest - h_two_two * second
    h_three_two = jnp.sqrt(jnp.sum(rest * rest) + epsilon)
    gram_aa = h_one_one * h_one_one + h_two_one * h_two_one
    gram_ab = h_one_one * h_one_two + h_two_one * h_two_two
    gram_bb = h_one_two * h_one_two + h_two_two * h_two_two + h_three_two * h_three_two
    right_a = beta * h_one_one
    right_b = beta * h_one_two
    determ = gram_aa * gram_bb - gram_ab * gram_ab
    coef_a = (gram_bb * right_a - gram_ab * right_b) / determ
    coef_b = (gram_aa * right_b - gram_ab * right_a) / determ
    solution = coef_a * first + coef_b * second
    residual = source - coef_a * image_one - coef_b * image_two
    return (solution, residual)
```

```python
import functools

import jax
import jax.numpy as jnp
from jax import lax
from jax.experimental import pallas as pl
from jax.experimental.pallas import tpu as pltpu
from jax.sharding import PartitionSpec as P

MESH = pl.DeviceIdType.MESH
HALO = 4
STRIDE = 2 * HALO + 1
LANES = 256
EPSILON = 1e-06
F32, BF16 = jnp.float32, jnp.bfloat16

PIECES = (
    (1, 0, 0, 0, 64),
    (-1, 0, 0, 128, 64),
    (0, 1, 2, 16, 16),
    (1, 1, 2, 0, 16),
    (-1, 1, 2, 32, 16),
    (0, -1, 1, 64, 16),
    (1, -1, 1, 48, 16),
    (-1, -1, 1, 80, 16),
)


def nt(a, b):
    return lax.dot_general(a, b, (((1,), (1,)), ((), ())), preferred_element_type=F32)


def nn(a, b):
    return lax.dot_general(a, b, (((1,), (0,)), ((), ())), preferred_element_type=F32)


def split(x):
    hi = x.astype(BF16)
    return hi, (x - hi.astype(F32)).astype(BF16)


def iota(shape, dim):
    return lax.broadcasted_iota(jnp.int32, shape, dim)


def kernel(
    ngx, ngy, inc_ref, kinds_ref, codes_ref, ops_ref, valid_ref, trans_hbm, tmat_hbm,
    sol_ref, res_ref,
    trans_v, tmat_v, tmhi, tmlo, tt, counts, grouped, mid, side, edge, vhi, vlo,
    one_out, one_in, two_out, two_in,
    load_sem, halo_send, halo_recv, ar_send, ar_recv,
):
    gx, gy = lax.axis_index("gx"), lax.axis_index("gy")
    rows, cols, coeffs = inc_ref.shape
    spheres = rows * cols
    slots = codes_ref.shape[2]
    count_ops, kinds_n = trans_v.shape[0], tmat_v.shape[0]

    def device(dx, dy):
        return (lax.rem(gx + (dx + ngx), ngx), lax.rem(gy + (dy + ngy), ngy))

    load_tm = pltpu.make_async_copy(tmat_hbm, tmat_v, load_sem.at[0])
    load_tm.start()
    load_tr = pltpu.make_async_copy(trans_hbm, trans_v, load_sem.at[1])
    load_tr.start()

    barrier = pltpu.get_barrier_semaphore()
    greeted = 0
    for dx, dy in [(0, d) for d in range(1, ngy)] + [(d, 0) for d in range(1, ngx)] + [
        (1, 1), (1, -1), (-1, 1), (-1, -1)
    ]:
        pl.semaphore_signal(barrier, inc=1, device_id=device(dx, dy), device_id_type=MESH)
        greeted += 1

    lane = iota((spheres, LANES), 1)
    eye = iota((cols, cols), 0) == iota((cols, cols), 1)
    kind_col = jnp.concatenate(
        [
            jnp.sum(
                jnp.where(eye, jnp.broadcast_to(kinds_ref[r : r + 1, :], (cols, cols)), 0).astype(F32),
                axis=1, keepdims=True,
            )
            for r in range(rows)
        ],
        axis=0,
    )

    def apply_kinds(u):
        total = None
        for p in range(kinds_n):
            hi, lo = split(jnp.where(kind_col == p, u, 0.0))
            term = nt(hi, tmhi[p]) + nt(lo, tmhi[p]) + nt(hi, tmlo[p])
            total = term if total is None else total + term
        return total

    def set_field(h, u):
        mid[h, spheres : 2 * spheres, :] = jnp.zeros((spheres, LANES), F32)
        mid[h, spheres : 2 * spheres, :coeffs] = u

        for r in range(rows):
            for e, c in ((0, 0), (1, cols - HALO)):
                edge[h, e, HALO * r : HALO * (r + 1), :] = mid[
                    h, spheres + cols * r + c : spheres + cols * r + c + HALO, :
                ]

    def exchange(h):
        copies = []
        for n, (dx, dy, source, first, count) in enumerate(PIECES):
            if source == 0:
                src, dst = mid.at[h, pl.ds(spheres, spheres)], mid.at[h, pl.ds(first, count)]
            else:
                src, dst = edge.at[h, source - 1], side.at[h, pl.ds(first, count)]
            copy = pltpu.make_async_remote_copy(
                src_ref=src, dst_ref=dst, send_sem=halo_send.at[h, n], recv_sem=halo_recv.at[h, n],
                device_id=device(dx, dy), device_id_type=MESH,
            )
            copy.start()
            copies.append(copy)
        return copies

    load_tm.wait()
    for p in range(kinds_n):
        hi, lo = split(tmat_v[p])
        tmhi[p] = hi
        tmlo[p] = lo
    set_field(0, apply_kinds(inc_ref[...].reshape(spheres, coeffs)))
    pl.semaphore_wait(barrier, greeted)
    flights = exchange(0)

    codes = codes_ref[...].reshape(spheres, slots)
    sphere = iota((spheres, slots), 0)
    row, col = sphere >> 4, sphere & 15
    step_x = (codes * 57) >> 9
    ext_x = row + step_x
    ext_y = col + codes - STRIDE * step_x
    target = jnp.where(
        ext_y < HALO,
        144 + HALO * ext_x + ext_y,
        jnp.where(ext_y < HALO + cols, cols * step_x + ext_y - HALO, 172 + HALO * ext_x + ext_y),
    )
    at_x = gx * rows + ext_x - HALO
    at_y = gy * cols + ext_y - HALO
    inside = (at_x >= 0) & (at_x < ngx * rows) & (at_y >= 0) & (at_y < ngy * cols)
    inside = inside & (valid_ref[...].reshape(spheres, slots) == 1)
    key = jnp.where(inside, row * count_ops + ops_ref[...].reshape(spheres, slots), -1)
    target = jnp.concatenate([target[cols * r : cols * (r + 1)] for r in range(rows)], axis=1)
    key = jnp.concatenate([key[cols * r : cols * (r + 1)] for r in range(rows)], axis=1)
    for c in range(cols):
        left = (iota((rows * count_ops, LANES), 0) == key[c : c + 1, :]).astype(F32).astype(BF16)
        right = (iota((LANES, LANES), 0) == target[c : c + 1, :]).astype(F32).astype(BF16)
        tally = nt(left, right)
        for r in range(rows):
            piece = tally[count_ops * r : count_ops * (r + 1)]
            for half in range(2):
                counts[half, pl.ds(r * cols * count_ops + c, count_ops, stride=cols), :] = piece[
                    :, 128 * half : 128 * (half + 1)
                ]

    load_tr.wait()
    unit = (iota((LANES, coeffs), 0) == iota((LANES, coeffs), 1)).astype(F32).astype(BF16)
    for k in range(count_ops):
        tt[k, :, :coeffs] = nt(unit, trans_v[k]).astype(BF16)

    def couple(h, copies):
        for copy in copies:
            copy.wait_recv()
        hi, lo = split(mid[h])
        vhi[: 3 * spheres], vlo[: 3 * spheres] = hi, lo
        hi, lo = split(side[h])
        vhi[3 * spheres :], vlo[3 * spheres :] = hi, lo
        tail = jnp.zeros((16, LANES), BF16)
        per_row = cols * count_ops
        for r in range(rows):
            table = jnp.concatenate(
                [counts[half, per_row * r : per_row * (r + 1), :].astype(BF16) for half in range(2)], axis=1
            )
            near = [
                jnp.concatenate([v[cols * r : cols * (r + STRIDE)], v[3 * spheres :], tail], axis=0)
                for v in (vhi, vlo)
            ]
            grouped[per_row * r : per_row * (r + 1), :] = nn(table, near[0]) + nn(table, near[1])
        total = None
        for k in range(count_ops):
            part = jnp.concatenate(
                [grouped[per_row * r + cols * k : per_row * r + cols * (k + 1), :] for r in range(rows)], axis=0
            )
            hi, lo = split(part)
            term = nn(jnp.concatenate([hi, lo], axis=0), tt[k])
            total = term if total is None else total + term
        moved = total[:spheres] + total[spheres:]
        return apply_kinds(moved[:, :coeffs])

    first_flights = flights
    set_field(1, couple(0, flights))
    flights = exchange(1)
    second = couple(1, flights)

    base = mid[0, spheres : 2 * spheres, :coeffs]
    once = mid[1, spheres : 2 * spheres, :coeffs]

    def inner(a, b):
        return jnp.sum(jnp.sum(a * b, axis=0, keepdims=True), axis=1, keepdims=True)

    products = (
        inner(base, base), inner(base, once), inner(once, once),
        inner(base, second), inner(once, second), inner(second, second),
    )
    slot = iota((1, 128), 1)
    packed = jnp.zeros((1, 128), F32)
    for n, value in enumerate(products):
        packed = jnp.where(slot == n, value, packed)

    def all_sum(n, value, out, into, peers):
        out[...] = value
        for d, peer in enumerate(peers):
            pltpu.make_async_remote_copy(
                src_ref=out, dst_ref=into.at[d], send_sem=ar_send.at[n], recv_sem=ar_recv.at[n],
                device_id=peer, device_id_type=MESH,
            ).start()
        pltpu.make_async_copy(into, into, ar_recv.at[n]).wait()
        total = value
        for d in range(len(peers)):
            total = total + into[d]
        return total

    packed = all_sum(0, packed, one_out, one_in, [device(0, d) for d in range(1, ngy)])
    packed = all_sum(1, packed, two_out, two_in, [device(d, 0) for d in range(1, ngx)])

    def entry(n):
        return jnp.sum(jnp.where(slot == n, packed, 0.0), axis=1, keepdims=True)

    g00, g01, g11, g02, g12, g22 = [entry(n) for n in range(6)]
    gram = ((g00, g01, g02), (g01, g11, g12), (g02, g12, g22))

    def pair(a, b):
        total = None
        for i in range(3):
            for j in range(3):
                if a[i] is not None and b[j] is not None:
                    term = a[i] * b[j] * gram[i][j]
                    total = term if total is None else total + term
        return total

    beta2 = g00 + EPSILON
    beta = jnp.sqrt(beta2)
    ib = 1.0 / beta
    shift = (g01 + EPSILON) * ib * ib
    h11 = (g00 - g01) * ib * ib
    rest = (shift * ib, -ib, None)
    h21 = jnp.sqrt(jnp.maximum(pair(rest, rest), 0.0) + EPSILON)
    q = ib / h21
    v1 = (ib, None, None)
    v2 = (shift * q, -q, None)
    m2 = (shift * q, -(1.0 + shift) * q, q)
    h12 = pair(m2, v1)
    left = (m2[0] - h12 * ib, m2[1], m2[2])
    h22 = pair(left, v2)
    left = (left[0] - h22 * v2[0], left[1] - h22 * v2[1], left[2])
    h32 = jnp.sqrt(jnp.maximum(pair(left, left), 0.0) + EPSILON)
    aa = h11 * h11 + h21 * h21
    ab = h11 * h12 + h21 * h22
    bb = h12 * h12 + h22 * h22 + h32 * h32
    ra, rb = beta * h11, beta * h12
    determ = aa * bb - ab * ab
    y1 = (bb * ra - ab * rb) / determ
    y2 = (aa * rb - ab * ra) / determ
    s0 = y1 * ib + y2 * v2[0]
    s1 = y2 * v2[1]
    r0 = 1.0 - s0
    r1 = y1 * ib - y2 * m2[1]
    r2 = -y2 * q
    sol_ref[...] = (s0 * base + s1 * once).reshape(rows, cols, coeffs)
    res_ref[...] = (r0 * base + r1 * once + r2 * second).reshape(rows, cols, coeffs)

    for copy in first_flights + flights:
        copy.wait_send()
    pltpu.make_async_copy(one_in, one_in, ar_send.at[0]).wait()
    pltpu.make_async_copy(two_in, two_in, ar_send.at[1]).wait()


def solution(mesh):
    ngx, ngy = mesh.shape["gx"], mesh.shape["gy"]

    def body(incident, sphere_kinds, pair_codes, operators, pair_valid, translations, tmatrices):
        rows, cols, coeffs = incident.shape
        spheres = rows * cols
        count_ops, kinds_n = translations.shape[0], tmatrices.shape[0]
        vmem = pl.BlockSpec(memory_space=pltpu.VMEM)
        hbm = pl.BlockSpec(memory_space=pltpu.HBM)
        return pl.pallas_call(
            functools.partial(kernel, ngx, ngy),
            out_shape=(jax.ShapeDtypeStruct(incident.shape, F32),) * 2,
            in_specs=[vmem] * 5 + [hbm] * 2,
            out_specs=(vmem, vmem),
            scratch_shapes=[
                pltpu.VMEM(translations.shape, BF16),
                pltpu.VMEM(tmatrices.shape, F32),
                pltpu.VMEM(tmatrices.shape, BF16),
                pltpu.VMEM(tmatrices.shape, BF16),
                pltpu.VMEM((count_ops, LANES, LANES), BF16),
                pltpu.VMEM((2, spheres * count_ops, 128), F32),
                pltpu.VMEM((spheres * count_ops, LANES), F32),
                pltpu.VMEM((2, 3 * spheres, LANES), F32),
                pltpu.VMEM((2, 96, LANES), F32),
                pltpu.VMEM((2, 2, 16, LANES), F32),
                pltpu.VMEM((3 * spheres + 96, LANES), BF16),
                pltpu.VMEM((3 * spheres + 96, LANES), BF16),
                pltpu.VMEM((1, 128), F32),
                pltpu.VMEM((ngy - 1, 1, 128), F32),
                pltpu.VMEM((1, 128), F32),
                pltpu.VMEM((ngx - 1, 1, 128), F32),
                pltpu.SemaphoreType.DMA((2,)),
                pltpu.SemaphoreType.DMA((2, len(PIECES))),
                pltpu.SemaphoreType.DMA((2, len(PIECES))),
                pltpu.SemaphoreType.DMA((2,)),
                pltpu.SemaphoreType.DMA((2,)),
            ],
            compiler_params=pltpu.CompilerParams(collective_id=0, has_side_effects=True),
        )(incident, sphere_kinds, pair_codes, operators, pair_valid, translations, tmatrices)

    here, line, table = P("gx", "gy", None), P("gx", "gy"), P()
    return jax.shard_map(
        body, mesh=mesh, in_specs=(here, line, here, here, here, table, table), out_specs=(here, here), check_vma=False
    )
```

```python
import functools

import jax
import jax.numpy as jnp
from jax import lax
from jax.experimental import pallas as pl
from jax.experimental.pallas import tpu as pltpu
from jax.sharding import PartitionSpec as P

MESH = pl.DeviceIdType.MESH
HALO = 4
STRIDE = 2 * HALO + 1
LANES = 256
EPSILON = 1e-06
F32, BF16 = jnp.float32, jnp.bfloat16

PIECES = (
    (1, 1, 2, 0, 16),
    (-1, 1, 2, 32, 16),
    (1, -1, 1, 48, 16),
    (-1, -1, 1, 80, 16),
    (0, 1, 2, 16, 16),
    (0, -1, 1, 64, 16),
    (1, 0, 0, 0, 64),
    (-1, 0, 0, 128, 64),
)


def nt(a, b):
    return lax.dot_general(a, b, (((1,), (1,)), ((), ())), preferred_element_type=F32)


def nn(a, b):
    return lax.dot_general(a, b, (((1,), (0,)), ((), ())), preferred_element_type=F32)


def split(x):
    hi = x.astype(BF16)
    return hi, (x - hi.astype(F32)).astype(BF16)


def iota(shape, dim):
    return lax.broadcasted_iota(jnp.int32, shape, dim)


def spread(n):
    steps, d = [], 1
    while d < n // 2:
        steps.append(d)
        d *= 2
    return steps


def kernel(
    ngx, ngy, inc_hbm, kinds_hbm, codes_hbm, ops_hbm, valid_hbm, trans_hbm, tmat_hbm,
    state, sums,
    inc_ref, kinds_ref, codes_ref, ops_ref, valid_ref, trans_v, tmat_v,
    tmhi, tmlo, tmhi_t, tmlo_t, masks, tt, counts, grouped, mid, side, edge, vhi, vlo,
    one_out, one_in, two_out, two_in,
    load_sem, halo_send, halo_recv, ar_send, ar_recv, spread_sem,
):
    gx, gy = lax.axis_index("gx"), lax.axis_index("gy")
    rows, cols, coeffs = inc_ref.shape
    spheres = rows * cols
    slots = codes_ref.shape[2]
    count_ops, kinds_n = trans_v.shape[0], tmat_v.shape[0]

    def device(dx, dy):
        return (lax.rem(gx + (dx + ngx), ngx), lax.rem(gy + (dy + ngy), ngy))
    barrier = pltpu.get_barrier_semaphore()
    for dx, dy, _, _, _ in PIECES:
        pl.semaphore_signal(barrier, inc=1, device_id=device(dx, dy), device_id_type=MESH)
    loads = []
    for n, (src, dst) in enumerate((
        (tmat_hbm, tmat_v), (inc_hbm, inc_ref), (kinds_hbm, kinds_ref), (codes_hbm, codes_ref),
        (ops_hbm, ops_ref), (valid_hbm, valid_ref), (trans_hbm, trans_v),
    )):
        loads.append(pltpu.make_async_copy(src, dst, load_sem.at[n]))
        loads[-1].start()

    rounds = [[(0, d) for d in spread(ngy)], [(d, 0) for d in spread(ngx)]]

    def tell(n):
        for axis, steps in enumerate(rounds):
            if n < len(steps):
                dx, dy = steps[n]
                for sign in (1, -1):
                    pl.semaphore_signal(
                        spread_sem.at[axis, n], inc=1, device_id=device(sign * dx, sign * dy), device_id_type=MESH
                    )

    def hear(n):
        for axis, steps in enumerate(rounds):
            if n < len(steps):
                pl.semaphore_wait(spread_sem.at[axis, n], 2)
    for n in range(3):
        loads[n].wait()
    lane = iota((spheres, LANES), 1)
    eye = iota((cols, cols), 0) == iota((cols, cols), 1)
    kind_col = jnp.concatenate(
        [
            jnp.sum(
                jnp.where(eye, jnp.broadcast_to(kinds_ref[r : r + 1, :], (cols, cols)), 0).astype(F32),
                axis=1, keepdims=True,
            )
            for r in range(rows)
        ],
        axis=0,
    )

    def source_of(u):
        total = None
        for p in range(kinds_n):
            hi, lo = split(jnp.where(kind_col == p, u, 0.0))
            term = nt(hi, tmhi[p]) + nt(lo, tmhi[p]) + nt(hi, tmlo[p])
            total = term if total is None else total + term
        return total

    def apply_kinds(u):
        hi, lo = split(u)
        both = jnp.concatenate([hi, lo], axis=0)
        wide, fine = None, None
        for p in range(kinds_n):
            chosen = both * masks[p]
            term, more = nn(chosen, tmhi_t[p]), nn(chosen[:spheres], tmlo_t[p])
            wide, fine = (term, more) if wide is None else (wide + term, fine + more)
        return jnp.where(lane < coeffs, wide[:spheres] + wide[spheres:] + fine, 0.0)

    def set_field(h, u):
        mid[h, spheres : 2 * spheres, :] = u
        state[h] = u
        for r in range(rows):
            for e, c in ((0, 0), (1, cols - HALO)):
                edge[h, e, HALO * r : HALO * (r + 1), :] = mid[
                    h, spheres + cols * r + c : spheres + cols * r + c + HALO, :
                ]

    def exchange(h):
        copies = []
        for n, (dx, dy, source, first, count) in enumerate(PIECES):
            if source == 0:
                src, dst = mid.at[h, pl.ds(spheres, spheres)], mid.at[h, pl.ds(first, count)]
            else:
                src, dst = edge.at[h, source - 1], side.at[h, pl.ds(first, count)]
            copy = pltpu.make_async_remote_copy(
                src_ref=src, dst_ref=dst, send_sem=halo_send.at[h, n], recv_sem=halo_recv.at[h, n],
                device_id=device(dx, dy), device_id_type=MESH,
            )
            copy.start()
            copies.append(copy)
        return copies

    for p in range(kinds_n):
        hi, lo = split(tmat_v[p])
        tmhi[p] = hi
        tmlo[p] = lo
    state[0] = jnp.zeros((spheres, LANES), F32)
    state[0, :, :coeffs] = source_of(inc_ref[...].reshape(spheres, coeffs))
    set_field(0, state[0])
    pl.semaphore_wait(barrier, len(PIECES))
    flights = exchange(0)
    tell(0)
    for n in range(3, 6):
        loads[n].wait()
    codes = codes_ref[...].reshape(spheres, slots)
    sphere = iota((spheres, slots), 0)
    row, col = sphere >> 4, sphere & 15
    step_x = (codes * 57) >> 9
    ext_x = row + step_x
    ext_y = col + codes - STRIDE * step_x
    target = jnp.where(
        ext_y < HALO,
        144 + HALO * ext_x + ext_y,
        jnp.where(ext_y < HALO + cols, cols * step_x + ext_y - HALO, 172 + HALO * ext_x + ext_y),
    )
    at_x = gx * rows + ext_x - HALO
    at_y = gy * cols + ext_y - HALO
    inside = (at_x >= 0) & (at_x < ngx * rows) & (at_y >= 0) & (at_y < ngy * cols)
    inside = inside & (valid_ref[...].reshape(spheres, slots) == 1)
    key = jnp.where(inside, row * count_ops + ops_ref[...].reshape(spheres, slots), -1)
    target = jnp.concatenate([target[cols * r : cols * (r + 1)] for r in range(rows)], axis=1)
    key = jnp.concatenate([key[cols * r : cols * (r + 1)] for r in range(rows)], axis=1)
    for c in range(cols):
        left = (iota((rows * count_ops, LANES), 0) == key[c : c + 1, :]).astype(F32).astype(BF16)
        right = (iota((LANES, LANES), 0) == target[c : c + 1, :]).astype(F32).astype(BF16)
        tally = nt(left, right)
        for r in range(rows):
            piece = tally[count_ops * r : count_ops * (r + 1)]
            for half in range(2):
                counts[half, pl.ds(r * cols * count_ops + c, count_ops, stride=cols), :] = piece[
                    :, 128 * half : 128 * (half + 1)
                ]

    loads[6].wait()
    hear(0)
    tell(1)
    unit = (iota((LANES, coeffs), 0) == iota((LANES, coeffs), 1)).astype(F32).astype(BF16)
    for k in range(count_ops):
        tt[k, :, :coeffs] = nt(unit, trans_v[k]).astype(BF16)
    for p in range(kinds_n):
        tmhi_t[p, :, :coeffs] = nt(unit, tmhi[p]).astype(BF16)
        tmlo_t[p, :, :coeffs] = nt(unit, tmlo[p]).astype(BF16)
        mask = jnp.where(jnp.broadcast_to(kind_col, (spheres, LANES)) == p, 1.0, 0.0)
        masks[p] = jnp.concatenate([mask, mask], axis=0).astype(BF16)
    hear(1)
    tell(2)
    def couple(h, copies):
        for copy in copies:
            copy.wait_recv()
        hi, lo = split(mid[h])
        vhi[: 3 * spheres], vlo[: 3 * spheres] = hi, lo
        hi, lo = split(side[h])
        vhi[3 * spheres :], vlo[3 * spheres :] = hi, lo
        tail = jnp.zeros((16, LANES), BF16)
        per_row = cols * count_ops
        for r in range(rows):
            table = jnp.concatenate(
                [counts[half, per_row * r : per_row * (r + 1), :].astype(BF16) for half in range(2)], axis=1
            )
            near = [
                jnp.concatenate([v[cols * r : cols * (r + STRIDE)], v[3 * spheres :], tail], axis=0)
                for v in (vhi, vlo)
            ]
            grouped[per_row * r : per_row * (r + 1), :] = nn(table, near[0]) + nn(table, near[1])
        total = None
        for k in range(count_ops):
            part = jnp.concatenate(
                [grouped[per_row * r + cols * k : per_row * r + cols * (k + 1), :] for r in range(rows)], axis=0
            )
            hi, lo = split(part)
            term = nn(jnp.concatenate([hi, lo], axis=0), tt[k])
            total = term if total is None else total + term
        moved = jnp.where(lane < coeffs, total[:spheres] + total[spheres:], 0.0)
        result = apply_kinds(moved)
        return result

    first_flights = flights
    once = couple(0, flights)
    set_field(1, once)
    flights = exchange(1)
    hear(2)
    tell(3)
    second = couple(1, flights)
    state[2] = second
    base, once = state[0], state[1]

    def inner(a, b):
        return jnp.sum(jnp.sum(a * b, axis=0, keepdims=True), axis=1, keepdims=True)

    products = (
        inner(base, base), inner(base, once), inner(once, once),
        inner(base, second), inner(once, second), inner(second, second),
    )
    slot = iota((1, 128), 1)
    packed = jnp.zeros((1, 128), F32)
    for n, value in enumerate(products):
        packed = jnp.where(slot == n, value, packed)
    def all_sum(n, value, out, into, peers):
        out[...] = value
        for d, peer in enumerate(peers):
            pltpu.make_async_remote_copy(
                src_ref=out, dst_ref=into.at[d], send_sem=ar_send.at[n], recv_sem=ar_recv.at[n],
                device_id=peer, device_id_type=MESH,
            ).start()
        pltpu.make_async_copy(into, into, ar_recv.at[n]).wait()
        total = value
        for d in range(len(peers)):
            total = total + into[d]
        return total

    def far_first(n, inner):
        def hops(d):
            return min(d // inner, n // inner - d // inner) + min(d % inner, inner - d % inner)

        return sorted(range(1, n), key=lambda d: -hops(d))
    hear(3)
    packed = all_sum(0, packed, one_out, one_in, [device(0, d) for d in far_first(ngy, 8)])
    packed = all_sum(1, packed, two_out, two_in, [device(d, 0) for d in far_first(ngx, 2)])
    sums[...] = packed
    for copy in first_flights + flights:
        copy.wait_send()
    pltpu.make_async_copy(one_in, one_in, ar_send.at[0]).wait()
    pltpu.make_async_copy(two_in, two_in, ar_send.at[1]).wait()


def combine(state, sums, sol_ref, res_ref):
    rows, cols, coeffs = sol_ref.shape
    packed = sums[...]
    slot = iota((1, 128), 1)
    base, once, second = [state[n][:, :coeffs] for n in range(3)]

    def entry(n):
        return jnp.sum(jnp.where(slot == n, packed, 0.0), axis=1, keepdims=True)

    g00, g01, g11, g02, g12, g22 = [entry(n) for n in range(6)]
    gram = ((g00, g01, g02), (g01, g11, g12), (g02, g12, g22))

    def pair(a, b):
        total = None
        for i in range(3):
            for j in range(3):
                if a[i] is not None and b[j] is not None:
                    term = a[i] * b[j] * gram[i][j]
                    total = term if total is None else total + term
        return total

    beta2 = g00 + EPSILON
    beta = jnp.sqrt(beta2)
    ib = 1.0 / beta
    shift = (g01 + EPSILON) * ib * ib
    h11 = (g00 - g01) * ib * ib
    rest = (shift * ib, -ib, None)
    h21 = jnp.sqrt(jnp.maximum(pair(rest, rest), 0.0) + EPSILON)
    q = ib / h21
    v1 = (ib, None, None)
    v2 = (shift * q, -q, None)
    m2 = (shift * q, -(1.0 + shift) * q, q)
    h12 = pair(m2, v1)
    left = (m2[0] - h12 * ib, m2[1], m2[2])
    h22 = pair(left, v2)
    left = (left[0] - h22 * v2[0], left[1] - h22 * v2[1], left[2])
    h32 = jnp.sqrt(jnp.maximum(pair(left, left), 0.0) + EPSILON)
    aa = h11 * h11 + h21 * h21
    ab = h11 * h12 + h21 * h22
    bb = h12 * h12 + h22 * h22 + h32 * h32
    ra, rb = beta * h11, beta * h12
    determ = aa * bb - ab * ab
    y1 = (bb * ra - ab * rb) / determ
    y2 = (aa * rb - ab * ra) / determ
    s0 = y1 * ib + y2 * v2[0]
    s1 = y2 * v2[1]
    r0 = 1.0 - s0
    r1 = y1 * ib - y2 * m2[1]
    r2 = -y2 * q
    sol_ref[...] = (s0 * base + s1 * once).reshape(rows, cols, coeffs)
    res_ref[...] = (r0 * base + r1 * once + r2 * second).reshape(rows, cols, coeffs)


def solution(mesh):
    ngx, ngy = mesh.shape["gx"], mesh.shape["gy"]

    def body(incident, sphere_kinds, pair_codes, operators, pair_valid, translations, tmatrices):
        rows, cols, coeffs = incident.shape
        spheres = rows * cols
        count_ops, kinds_n = translations.shape[0], tmatrices.shape[0]
        vmem = pl.BlockSpec(memory_space=pltpu.VMEM)
        hbm = pl.BlockSpec(memory_space=pltpu.HBM)
        args = (incident, sphere_kinds, pair_codes, operators, pair_valid, translations, tmatrices)
        state, sums = pl.pallas_call(
            functools.partial(kernel, ngx, ngy),
            out_shape=(pltpu.VMEM((3, spheres, LANES), F32), pltpu.VMEM((1, 128), F32)),
            in_specs=[hbm] * 7,
            out_specs=(vmem, vmem),
            scratch_shapes=[pltpu.VMEM(arg.shape, arg.dtype) for arg in args]
            + [pltpu.VMEM(tmatrices.shape, BF16)] * 2
            + [pltpu.VMEM((kinds_n, LANES, LANES), BF16)] * 2
            + [
                pltpu.VMEM((kinds_n, 2 * spheres, LANES), BF16),
                pltpu.VMEM((count_ops, LANES, LANES), BF16),
                pltpu.VMEM((2, spheres * count_ops, 128), F32),
                pltpu.VMEM((spheres * count_ops, LANES), F32),
                pltpu.VMEM((2, 3 * spheres, LANES), F32),
                pltpu.VMEM((2, 96, LANES), F32),
                pltpu.VMEM((2, 2, 16, LANES), F32),
                pltpu.VMEM((3 * spheres + 96, LANES), BF16),
                pltpu.VMEM((3 * spheres + 96, LANES), BF16),
                pltpu.VMEM((1, 128), F32),
                pltpu.VMEM((ngy - 1, 1, 128), F32),
                pltpu.VMEM((1, 128), F32),
                pltpu.VMEM((ngx - 1, 1, 128), F32),
                pltpu.SemaphoreType.DMA((7,)),
                pltpu.SemaphoreType.DMA((2, len(PIECES))),
                pltpu.SemaphoreType.DMA((2, len(PIECES))),
                pltpu.SemaphoreType.DMA((2,)),
                pltpu.SemaphoreType.DMA((2,)),
                pltpu.SemaphoreType.REGULAR((2, 4)),
            ],
            compiler_params=pltpu.CompilerParams(collective_id=0, has_side_effects=True),
        )(*args)
        state, sums = [pltpu.with_memory_space_constraint(x, pltpu.VMEM) for x in (state, sums)]
        return pl.pallas_call(
            combine,
            out_shape=(jax.ShapeDtypeStruct(incident.shape, F32),) * 2,
            in_specs=[vmem] * 2,
            out_specs=(vmem, vmem),
        )(state, sums)

    here, line, table = P("gx", "gy", None), P("gx", "gy"), P()
    return jax.shard_map(
        body, mesh=mesh, in_specs=(here, line, here, here, here, table, table), out_specs=(here, here), check_vma=False
    )
```

```python
import functools

import jax
import jax.numpy as jnp
from jax import lax
from jax.experimental import pallas as pl
from jax.experimental.pallas import tpu as pltpu
from jax.sharding import PartitionSpec as P

MESH = pl.DeviceIdType.MESH
HALO = 4
STRIDE = 2 * HALO + 1
LANES = 256
EPSILON = 1e-06
F32, BF16 = jnp.float32, jnp.bfloat16

PIECES = (
    (1, 1, 2, 0, 16),
    (-1, 1, 2, 32, 16),
    (1, -1, 1, 48, 16),
    (-1, -1, 1, 80, 16),
    (0, 1, 2, 16, 16),
    (0, -1, 1, 64, 16),
    (1, 0, 0, 0, 64),
    (-1, 0, 0, 128, 64),
)


def nt(a, b):
    return lax.dot_general(a, b, (((1,), (1,)), ((), ())), preferred_element_type=F32)


def nn(a, b):
    return lax.dot_general(a, b, (((1,), (0,)), ((), ())), preferred_element_type=F32)


def split(x):
    hi = x.astype(BF16)
    return hi, (x - hi.astype(F32)).astype(BF16)


def iota(shape, dim):
    return lax.broadcasted_iota(jnp.int32, shape, dim)


def spread(n):
    steps, d = [], 1
    while d < n // 2:
        steps.append(d)
        d *= 2
    return steps


def kernel(
    ngx, ngy, inc_hbm, kinds_hbm, codes_hbm, ops_hbm, valid_hbm, trans_hbm, tmat_hbm,
    state, sums,
    inc_ref, kinds_ref, codes_ref, ops_ref, valid_ref, trans_v, tmat_v,
    tmhi, tmlo, tmhi_t, tmlo_t, masks, tt, counts, grouped, mid, side, edge, vhi, vlo,
    one_out, one_in, two_out, two_in,
    load_sem, halo_send, halo_recv, ar_send, ar_recv, spread_sem,
):
    gx, gy = lax.axis_index("gx"), lax.axis_index("gy")
    rows, cols, coeffs = inc_ref.shape
    spheres = rows * cols
    slots = codes_ref.shape[2]
    count_ops, kinds_n = trans_v.shape[0], tmat_v.shape[0]

    def device(dx, dy):
        return (lax.rem(gx + (dx + ngx), ngx), lax.rem(gy + (dy + ngy), ngy))
    barrier = pltpu.get_barrier_semaphore()
    for dx, dy, _, _, _ in PIECES:
        pl.semaphore_signal(barrier, inc=1, device_id=device(dx, dy), device_id_type=MESH)
    loads = []
    for n, (src, dst) in enumerate((
        (tmat_hbm, tmat_v), (inc_hbm, inc_ref), (kinds_hbm, kinds_ref), (codes_hbm, codes_ref),
        (ops_hbm, ops_ref), (valid_hbm, valid_ref), (trans_hbm, trans_v),
    )):
        loads.append(pltpu.make_async_copy(src, dst, load_sem.at[n]))
    for n in range(3):
        loads[n].start()

    rounds = [[(0, d) for d in spread(ngy)], [(d, 0) for d in spread(ngx)]]

    def tell(n):
        for axis, steps in enumerate(rounds):
            if n < len(steps):
                dx, dy = steps[n]
                for sign in (1, -1):
                    pl.semaphore_signal(
                        spread_sem.at[axis, n], inc=1, device_id=device(sign * dx, sign * dy), device_id_type=MESH
                    )

    def hear(n):
        for axis, steps in enumerate(rounds):
            if n < len(steps):
                pl.semaphore_wait(spread_sem.at[axis, n], 2)
    for n in range(3):
        loads[n].wait()
    for n in range(3, 7):
        loads[n].start()
    lane = iota((spheres, LANES), 1)
    eye = iota((cols, cols), 0) == iota((cols, cols), 1)
    kind_col = jnp.concatenate(
        [
            jnp.sum(
                jnp.where(eye, jnp.broadcast_to(kinds_ref[r : r + 1, :], (cols, cols)), 0).astype(F32),
                axis=1, keepdims=True,
            )
            for r in range(rows)
        ],
        axis=0,
    )

    def source_of(u):
        total = None
        for p in range(kinds_n):
            hi, lo = split(jnp.where(kind_col == p, u, 0.0))
            term = nt(hi, tmhi[p]) + nt(lo, tmhi[p]) + nt(hi, tmlo[p])
            total = term if total is None else total + term
        return total

    def apply_kinds(u):
        hi, lo = split(u)
        both = jnp.concatenate([hi, lo], axis=0)
        wide, fine = None, None
        for p in range(kinds_n):
            chosen = both * masks[p]
            term, more = nn(chosen, tmhi_t[p]), nn(chosen[:spheres], tmlo_t[p])
            wide, fine = (term, more) if wide is None else (wide + term, fine + more)
        return jnp.where(lane < coeffs, wide[:spheres] + wide[spheres:] + fine, 0.0)

    def set_field(h, u):
        mid[h, spheres : 2 * spheres, :] = u
        state[h] = u
        for r in range(rows):
            for e, c in ((0, 0), (1, cols - HALO)):
                edge[h, e, HALO * r : HALO * (r + 1), :] = mid[
                    h, spheres + cols * r + c : spheres + cols * r + c + HALO, :
                ]

    def exchange(h):
        copies = []
        for n, (dx, dy, source, first, count) in enumerate(PIECES):
            if source == 0:
                src, dst = mid.at[h, pl.ds(spheres, spheres)], mid.at[h, pl.ds(first, count)]
            else:
                src, dst = edge.at[h, source - 1], side.at[h, pl.ds(first, count)]
            copy = pltpu.make_async_remote_copy(
                src_ref=src, dst_ref=dst, send_sem=halo_send.at[h, n], recv_sem=halo_recv.at[h, n],
                device_id=device(dx, dy), device_id_type=MESH,
            )
            copy.start()
            copies.append(copy)
        return copies

    for p in range(kinds_n):
        hi, lo = split(tmat_v[p])
        tmhi[p] = hi
        tmlo[p] = lo
    state[0] = jnp.zeros((spheres, LANES), F32)
    state[0, :, :coeffs] = source_of(inc_ref[...].reshape(spheres, coeffs))
    set_field(0, state[0])
    pl.semaphore_wait(barrier, len(PIECES))
    flights = exchange(0)
    tell(0)
    for n in range(3, 6):
        loads[n].wait()
    codes = codes_ref[...].reshape(spheres, slots)
    sphere = iota((spheres, slots), 0)
    row, col = sphere >> 4, sphere & 15
    step_x = (codes * 57) >> 9
    ext_x = row + step_x
    ext_y = col + codes - STRIDE * step_x
    target = jnp.where(
        ext_y < HALO,
        144 + HALO * ext_x + ext_y,
        jnp.where(ext_y < HALO + cols, cols * step_x + ext_y - HALO, 172 + HALO * ext_x + ext_y),
    )
    at_x = gx * rows + ext_x - HALO
    at_y = gy * cols + ext_y - HALO
    inside = (at_x >= 0) & (at_x < ngx * rows) & (at_y >= 0) & (at_y < ngy * cols)
    inside = inside & (valid_ref[...].reshape(spheres, slots) == 1)
    key = jnp.where(inside, row * count_ops + ops_ref[...].reshape(spheres, slots), -1)
    target = jnp.concatenate([target[cols * r : cols * (r + 1)] for r in range(rows)], axis=1)
    key = jnp.concatenate([key[cols * r : cols * (r + 1)] for r in range(rows)], axis=1)
    for c in range(cols):
        left = (iota((rows * count_ops, LANES), 0) == key[c : c + 1, :]).astype(F32).astype(BF16)
        right = (iota((LANES, LANES), 0) == target[c : c + 1, :]).astype(F32).astype(BF16)
        tally = nt(left, right)
        for r in range(rows):
            piece = tally[count_ops * r : count_ops * (r + 1)]
            for half in range(2):
                counts[half, pl.ds(r * cols * count_ops + c, count_ops, stride=cols), :] = piece[
                    :, 128 * half : 128 * (half + 1)
                ]

    loads[6].wait()
    unit = (iota((LANES, coeffs), 0) == iota((LANES, coeffs), 1)).astype(F32).astype(BF16)
    for k in range(count_ops):
        tt[k, :, :coeffs] = nt(unit, trans_v[k]).astype(BF16)
    for p in range(kinds_n):
        tmhi_t[p, :, :coeffs] = nt(unit, tmhi[p]).astype(BF16)
        tmlo_t[p, :, :coeffs] = nt(unit, tmlo[p]).astype(BF16)
        mask = jnp.where(jnp.broadcast_to(kind_col, (spheres, LANES)) == p, 1.0, 0.0)
        masks[p] = jnp.concatenate([mask, mask], axis=0).astype(BF16)
    def couple(h, copies):
        for copy in copies:
            copy.wait_recv()
        hear(2 * h)
        tell(2 * h + 1)
        hi, lo = split(mid[h])
        vhi[: 3 * spheres], vlo[: 3 * spheres] = hi, lo
        hi, lo = split(side[h])
        vhi[3 * spheres :], vlo[3 * spheres :] = hi, lo
        tail = jnp.zeros((16, LANES), BF16)
        per_row = cols * count_ops
        for r in range(rows):
            table = jnp.concatenate(
                [counts[half, per_row * r : per_row * (r + 1), :].astype(BF16) for half in range(2)], axis=1
            )
            near = [
                jnp.concatenate([v[cols * r : cols * (r + STRIDE)], v[3 * spheres :], tail], axis=0)
                for v in (vhi, vlo)
            ]
            grouped[per_row * r : per_row * (r + 1), :] = nn(table, near[0]) + nn(table, near[1])
        total = None
        for k in range(count_ops):
            part = jnp.concatenate(
                [grouped[per_row * r + cols * k : per_row * r + cols * (k + 1), :] for r in range(rows)], axis=0
            )
            hi, lo = split(part)
            term = nn(jnp.concatenate([hi, lo], axis=0), tt[k])
            total = term if total is None else total + term
        moved = jnp.where(lane < coeffs, total[:spheres] + total[spheres:], 0.0)
        result = apply_kinds(moved)
        return result

    first_flights = flights
    once = couple(0, flights)
    set_field(1, once)
    flights = exchange(1)
    hear(1)
    tell(2)
    second = couple(1, flights)
    state[2] = second
    base, once = state[0], state[1]

    def inner(a, b):
        return jnp.sum(jnp.sum(a * b, axis=0, keepdims=True), axis=1, keepdims=True)

    products = (
        inner(base, base), inner(base, once), inner(once, once),
        inner(base, second), inner(once, second), inner(second, second),
    )
    slot = iota((1, 128), 1)
    packed = jnp.zeros((1, 128), F32)
    for n, value in enumerate(products):
        packed = jnp.where(slot == n, value, packed)
    core = lax.rem(gx, 2)
    chips, group = ngx // 2, one_in.shape[0]

    def far_first(n, inner):
        def hops(d):
            return min(d // inner, n // inner - d // inner) + min(d % inner, inner - d % inner)

        return sorted(range(1, n), key=lambda d: -hops(d))

    def along_x(d):
        return (lax.rem(gx - core + 2 * d + 1, ngx), gy)

    def send(n, out, into, slot, peer):
        pltpu.make_async_remote_copy(
            src_ref=out, dst_ref=into.at[slot], send_sem=ar_send.at[n], recv_sem=ar_recv.at[n],
            device_id=peer, device_id_type=MESH,
        ).start()
    one_out[...] = packed
    for d in far_first(chips, 1):

        @pl.when(core == 1)
        def _():
            send(0, one_out, one_in, d - 1, along_x(d))

        @pl.when(core == 0)
        def _():
            send(0, one_out, one_in, chips - 1 + d, along_x(d))

    @pl.when(core == 0)
    def _():
        send(0, one_out, one_in, chips - 1, along_x(0))

    hear(3)

    @pl.when(core == 1)
    def _():
        pltpu.make_async_copy(one_in, one_in, ar_recv.at[0]).wait()
        total = one_out[...]
        for n in range(group):
            total = total + one_in[n]
        two_out[...] = total
        for c in (-1, 0):
            for d in far_first(ngy, 8):
                send(1, two_out, two_in, d, (gx + c, lax.rem(gy + d, ngy)))
        send(1, two_out, two_in, 0, (gx - 1, gy))
        two_in[0] = total
        far = two_in.at[pl.ds(1, ngy - 1)]
        pltpu.make_async_copy(far, far, ar_recv.at[1]).wait()
        out = one_in.at[pl.ds(0, chips - 1)]
        pltpu.make_async_copy(out, out, ar_send.at[0]).wait()
        pltpu.make_async_copy(two_in, two_in, ar_send.at[1]).wait()
        pltpu.make_async_copy(far, far, ar_send.at[1]).wait()
    @pl.when(core == 0)
    def _():
        pltpu.make_async_copy(two_in, two_in, ar_recv.at[1]).wait()
        out = one_in.at[pl.ds(0, chips)]
        pltpu.make_async_copy(out, out, ar_send.at[0]).wait()

    packed = two_in[0]
    for n in range(1, ngy):
        packed = packed + two_in[n]
    sums[...] = packed
    for copy in first_flights + flights:
        copy.wait_send()


def combine(state, sums, sol_ref, res_ref):
    rows, cols, coeffs = sol_ref.shape
    packed = sums[...]
    slot = iota((1, 128), 1)
    base, once, second = [state[n][:, :coeffs] for n in range(3)]

    def entry(n):
        return jnp.sum(jnp.where(slot == n, packed, 0.0), axis=1, keepdims=True)

    g00, g01, g11, g02, g12, g22 = [entry(n) for n in range(6)]
    gram = ((g00, g01, g02), (g01, g11, g12), (g02, g12, g22))

    def pair(a, b):
        total = None
        for i in range(3):
            for j in range(3):
                if a[i] is not None and b[j] is not None:
                    term = a[i] * b[j] * gram[i][j]
                    total = term if total is None else total + term
        return total

    beta2 = g00 + EPSILON
    beta = jnp.sqrt(beta2)
    ib = 1.0 / beta
    shift = (g01 + EPSILON) * ib * ib
    h11 = (g00 - g01) * ib * ib
    rest = (shift * ib, -ib, None)
    h21 = jnp.sqrt(jnp.maximum(pair(rest, rest), 0.0) + EPSILON)
    q = ib / h21
    v1 = (ib, None, None)
    v2 = (shift * q, -q, None)
    m2 = (shift * q, -(1.0 + shift) * q, q)
    h12 = pair(m2, v1)
    left = (m2[0] - h12 * ib, m2[1], m2[2])
    h22 = pair(left, v2)
    left = (left[0] - h22 * v2[0], left[1] - h22 * v2[1], left[2])
    h32 = jnp.sqrt(jnp.maximum(pair(left, left), 0.0) + EPSILON)
    aa = h11 * h11 + h21 * h21
    ab = h11 * h12 + h21 * h22
    bb = h12 * h12 + h22 * h22 + h32 * h32
    ra, rb = beta * h11, beta * h12
    determ = aa * bb - ab * ab
    y1 = (bb * ra - ab * rb) / determ
    y2 = (aa * rb - ab * ra) / determ
    s0 = y1 * ib + y2 * v2[0]
    s1 = y2 * v2[1]
    r0 = 1.0 - s0
    r1 = y1 * ib - y2 * m2[1]
    r2 = -y2 * q
    sol_ref[...] = (s0 * base + s1 * once).reshape(rows, cols, coeffs)
    res_ref[...] = (r0 * base + r1 * once + r2 * second).reshape(rows, cols, coeffs)


def solution(mesh):
    ngx, ngy = mesh.shape["gx"], mesh.shape["gy"]

    def body(incident, sphere_kinds, pair_codes, operators, pair_valid, translations, tmatrices):
        rows, cols, coeffs = incident.shape
        spheres = rows * cols
        count_ops, kinds_n = translations.shape[0], tmatrices.shape[0]
        vmem = pl.BlockSpec(memory_space=pltpu.VMEM)
        hbm = pl.BlockSpec(memory_space=pltpu.HBM)
        args = (incident, sphere_kinds, pair_codes, operators, pair_valid, translations, tmatrices)
        state, sums = pl.pallas_call(
            functools.partial(kernel, ngx, ngy),
            out_shape=(pltpu.VMEM((3, spheres, LANES), F32), pltpu.VMEM((1, 128), F32)),
            in_specs=[hbm] * 7,
            out_specs=(vmem, vmem),
            scratch_shapes=[pltpu.VMEM(arg.shape, arg.dtype) for arg in args]
            + [pltpu.VMEM(tmatrices.shape, BF16)] * 2
            + [pltpu.VMEM((kinds_n, LANES, LANES), BF16)] * 2
            + [
                pltpu.VMEM((kinds_n, 2 * spheres, LANES), BF16),
                pltpu.VMEM((count_ops, LANES, LANES), BF16),
                pltpu.VMEM((2, spheres * count_ops, 128), F32),
                pltpu.VMEM((spheres * count_ops, LANES), F32),
                pltpu.VMEM((2, 3 * spheres, LANES), F32),
                pltpu.VMEM((2, 96, LANES), F32),
                pltpu.VMEM((2, 2, 16, LANES), F32),
                pltpu.VMEM((3 * spheres + 96, LANES), BF16),
                pltpu.VMEM((3 * spheres + 96, LANES), BF16),
                pltpu.VMEM((1, 128), F32),
                pltpu.VMEM((ngx - 1, 1, 128), F32),
                pltpu.VMEM((1, 128), F32),
                pltpu.VMEM((ngy, 1, 128), F32),
                pltpu.SemaphoreType.DMA((7,)),
                pltpu.SemaphoreType.DMA((2, len(PIECES))),
                pltpu.SemaphoreType.DMA((2, len(PIECES))),
                pltpu.SemaphoreType.DMA((2,)),
                pltpu.SemaphoreType.DMA((2,)),
                pltpu.SemaphoreType.REGULAR((2, 4)),
            ],
            compiler_params=pltpu.CompilerParams(collective_id=0, has_side_effects=True),
        )(*args)
        state, sums = [pltpu.with_memory_space_constraint(x, pltpu.VMEM) for x in (state, sums)]
        return pl.pallas_call(
            combine,
            out_shape=(jax.ShapeDtypeStruct(incident.shape, F32),) * 2,
            in_specs=[vmem] * 2,
            out_specs=(vmem, vmem),
        )(state, sums)

    here, line, table = P("gx", "gy", None), P("gx", "gy"), P()
    return jax.shard_map(
        body, mesh=mesh, in_specs=(here, line, here, here, here, table, table), out_specs=(here, here), check_vma=False
    )
```

```python
import functools

import jax
import jax.numpy as jnp
from jax import lax
from jax.experimental import pallas as pl
from jax.experimental.pallas import tpu as pltpu
from jax.sharding import PartitionSpec as P

MESH = pl.DeviceIdType.MESH
HALO = 4
STRIDE = 2 * HALO + 1
LANES = 256
EPSILON = 1e-06
F32, BF16 = jnp.float32, jnp.bfloat16

PIECES = (
    (1, 1, 2, 0, 16),
    (-1, 1, 2, 32, 16),
    (1, -1, 1, 48, 16),
    (-1, -1, 1, 80, 16),
    (0, 1, 2, 16, 16),
    (0, -1, 1, 64, 16),
    (1, 0, 0, 0, 64),
    (-1, 0, 0, 128, 64),
)


def nt(a, b):
    return lax.dot_general(a, b, (((1,), (1,)), ((), ())), preferred_element_type=F32)


def nn(a, b):
    return lax.dot_general(a, b, (((1,), (0,)), ((), ())), preferred_element_type=F32)


def split(x):
    hi = x.astype(BF16)
    return hi, (x - hi.astype(F32)).astype(BF16)


def iota(shape, dim):
    return lax.broadcasted_iota(jnp.int32, shape, dim)


def spread(n):
    steps, d = [], 1
    while d < n - 1:
        steps.append(d)
        d *= 2
    return steps


def kernel(
    ngx, ngy, inc_hbm, kinds_hbm, codes_hbm, ops_hbm, valid_hbm, trans_hbm, tmat_hbm,
    state, sums,
    inc_ref, kinds_ref, codes_ref, ops_ref, valid_ref, trans_v, tmat_v,
    tmhi, tmlo, tmhi_t, tmlo_t, masks, tt, counts, grouped, mid, side, edge, vhi, vlo,
    one_out, one_in, two_out, two_in,
    load_sem, halo_send, halo_recv, ar_send, ar_recv, spread_sem,
):
    gx, gy = lax.axis_index("gx"), lax.axis_index("gy")
    rows, cols, coeffs = inc_ref.shape
    spheres = rows * cols
    slots = codes_ref.shape[2]
    count_ops, kinds_n = trans_v.shape[0], tmat_v.shape[0]

    def device(dx, dy):
        return (lax.rem(gx + (dx + ngx), ngx), lax.rem(gy + (dy + ngy), ngy))

    def inside_tests(dx, dy):
        tests = []
        for at, n, d in ((gx, ngx, dx), (gy, ngy, dy)):
            if d > 0:
                tests.append(at < n - d)
            elif d < 0:
                tests.append(at >= -d)
        return tests

    def when(dx, dy):
        return pl.when(functools.reduce(jnp.logical_and, inside_tests(dx, dy)))

    def count_at(at, size, d):
        return (at >= d).astype(jnp.int32) + (at < size - d).astype(jnp.int32)

    def there(dx, dy):
        return (gx + dx, gy + dy)
    barrier = pltpu.get_barrier_semaphore()
    for dx, dy, _, _, _ in PIECES:

        @when(dx, dy)
        def _():
            pl.semaphore_signal(barrier, inc=1, device_id=there(dx, dy), device_id_type=MESH)

    loads = []
    for n, (src, dst) in enumerate((
        (tmat_hbm, tmat_v), (inc_hbm, inc_ref), (kinds_hbm, kinds_ref), (codes_hbm, codes_ref),
        (ops_hbm, ops_ref), (valid_hbm, valid_ref), (trans_hbm, trans_v),
    )):
        loads.append(pltpu.make_async_copy(src, dst, load_sem.at[n]))
    for n in range(3):
        loads[n].start()

    rounds = [[(0, d) for d in spread(ngy)], [(d, 0) for d in spread(ngx)]]

    def tell(n):
        for axis, steps in enumerate(rounds):
            if n < len(steps):
                dx, dy = steps[n]
                for sign in (1, -1):

                    @when(sign * dx, sign * dy)
                    def _():
                        pl.semaphore_signal(
                            spread_sem.at[axis, n], inc=1, device_id=there(sign * dx, sign * dy), device_id_type=MESH
                        )


    def hear(n):
        for axis, steps in enumerate(rounds):
            if n < len(steps):
                at, size = ((gy, ngy), (gx, ngx))[axis]
                pl.semaphore_wait(spread_sem.at[axis, n], count_at(at, size, sum(steps[n])))
    for n in range(3):
        loads[n].wait()
    for n in range(3, 7):
        loads[n].start()
    lane = iota((spheres, LANES), 1)
    eye = iota((cols, cols), 0) == iota((cols, cols), 1)
    kind_col = jnp.concatenate(
        [
            jnp.sum(
                jnp.where(eye, jnp.broadcast_to(kinds_ref[r : r + 1, :], (cols, cols)), 0).astype(F32),
                axis=1, keepdims=True,
            )
            for r in range(rows)
        ],
        axis=0,
    )

    def source_of(u):
        total = None
        for p in range(kinds_n):
            hi, lo = split(jnp.where(kind_col == p, u, 0.0))
            term = nt(hi, tmhi[p]) + nt(lo, tmhi[p]) + nt(hi, tmlo[p])
            total = term if total is None else total + term
        return total

    def apply_kinds(u):
        hi, lo = split(u)
        both = jnp.concatenate([hi, lo], axis=0)
        wide, fine = None, None
        for p in range(kinds_n):
            chosen = both * masks[p]
            term, more = nn(chosen, tmhi_t[p]), nn(chosen[:spheres], tmlo_t[p])
            wide, fine = (term, more) if wide is None else (wide + term, fine + more)
        return jnp.where(lane < coeffs, wide[:spheres] + wide[spheres:] + fine, 0.0)

    def set_field(h, u):
        mid[h, spheres : 2 * spheres, :] = u
        state[h] = u
        for r in range(rows):
            for e, c in ((0, 0), (1, cols - HALO)):
                edge[h, e, HALO * r : HALO * (r + 1), :] = mid[
                    h, spheres + cols * r + c : spheres + cols * r + c + HALO, :
                ]

    def pieces(h):
        for n, (dx, dy, source, first, count) in enumerate(PIECES):
            if source == 0:
                src, dst = mid.at[h, pl.ds(spheres, spheres)], mid.at[h, pl.ds(first, count)]
            else:
                src, dst = edge.at[h, source - 1], side.at[h, pl.ds(first, count)]
            copy = pltpu.make_async_remote_copy(
                src_ref=src, dst_ref=dst, send_sem=halo_send.at[h, n], recv_sem=halo_recv.at[h, n],
                device_id=there(dx, dy), device_id_type=MESH,
            )
            yield dx, dy, copy

    def exchange(h):
        for dx, dy, copy in pieces(h):
            when(dx, dy)(copy.start)

    def arrive(h):
        for dx, dy, copy in pieces(h):
            when(-dx, -dy)(copy.wait_recv)

    def sent(h):
        for dx, dy, copy in pieces(h):
            when(dx, dy)(copy.wait_send)

    for dx, dy, source, first, count in PIECES:

        @pl.when(jnp.logical_not(functools.reduce(jnp.logical_and, inside_tests(-dx, -dy))))
        def _():
            for h in range(2):
                (mid if source == 0 else side)[h, first : first + count, :] = jnp.zeros((count, LANES), F32)

    for p in range(kinds_n):
        hi, lo = split(tmat_v[p])
        tmhi[p] = hi
        tmlo[p] = lo
    state[0] = jnp.zeros((spheres, LANES), F32)
    state[0, :, :coeffs] = source_of(inc_ref[...].reshape(spheres, coeffs))
    set_field(0, state[0])
    near_x, near_y = count_at(gx, ngx, 1), count_at(gy, ngy, 1)
    pl.semaphore_wait(barrier, (near_x + 1) * (near_y + 1) - 1)
    exchange(0)
    tell(0)
    for n in range(3, 6):
        loads[n].wait()
    codes = codes_ref[...].reshape(spheres, slots)
    sphere = iota((spheres, slots), 0)
    row, col = sphere >> 4, sphere & 15
    step_x = (codes * 57) >> 9
    ext_x = row + step_x
    ext_y = col + codes - STRIDE * step_x
    target = jnp.where(
        ext_y < HALO,
        144 + HALO * ext_x + ext_y,
        jnp.where(ext_y < HALO + cols, cols * step_x + ext_y - HALO, 172 + HALO * ext_x + ext_y),
    )
    at_x = gx * rows + ext_x - HALO
    at_y = gy * cols + ext_y - HALO
    inside = (at_x >= 0) & (at_x < ngx * rows) & (at_y >= 0) & (at_y < ngy * cols)
    inside = inside & (valid_ref[...].reshape(spheres, slots) == 1)
    key = jnp.where(inside, row * count_ops + ops_ref[...].reshape(spheres, slots), -1)
    target = jnp.concatenate([target[cols * r : cols * (r + 1)] for r in range(rows)], axis=1)
    key = jnp.concatenate([key[cols * r : cols * (r + 1)] for r in range(rows)], axis=1)
    for c in range(cols):
        left = (iota((rows * count_ops, LANES), 0) == key[c : c + 1, :]).astype(F32).astype(BF16)
        right = (iota((LANES, LANES), 0) == target[c : c + 1, :]).astype(F32).astype(BF16)
        tally = nt(left, right)
        for r in range(rows):
            piece = tally[count_ops * r : count_ops * (r + 1)]
            for half in range(2):
                counts[half, pl.ds(r * cols * count_ops + c, count_ops, stride=cols), :] = piece[
                    :, 128 * half : 128 * (half + 1)
                ]

    loads[6].wait()
    unit = (iota((LANES, coeffs), 0) == iota((LANES, coeffs), 1)).astype(F32).astype(BF16)
    for k in range(count_ops):
        tt[k, :, :coeffs] = nt(unit, trans_v[k]).astype(BF16)
    for p in range(kinds_n):
        tmhi_t[p, :, :coeffs] = nt(unit, tmhi[p]).astype(BF16)
        tmlo_t[p, :, :coeffs] = nt(unit, tmlo[p]).astype(BF16)
        mask = jnp.where(jnp.broadcast_to(kind_col, (spheres, LANES)) == p, 1.0, 0.0)
        masks[p] = jnp.concatenate([mask, mask], axis=0).astype(BF16)
    def couple(h):
        arrive(h)
        hear(2 * h)
        tell(2 * h + 1)
        hi, lo = split(mid[h])
        vhi[: 3 * spheres], vlo[: 3 * spheres] = hi, lo
        hi, lo = split(side[h])
        vhi[3 * spheres :], vlo[3 * spheres :] = hi, lo
        tail = jnp.zeros((16, LANES), BF16)
        per_row = cols * count_ops
        for r in range(rows):
            table = jnp.concatenate(
                [counts[half, per_row * r : per_row * (r + 1), :].astype(BF16) for half in range(2)], axis=1
            )
            near = [
                jnp.concatenate([v[cols * r : cols * (r + STRIDE)], v[3 * spheres :], tail], axis=0)
                for v in (vhi, vlo)
            ]
            grouped[per_row * r : per_row * (r + 1), :] = nn(table, near[0]) + nn(table, near[1])
        total = None
        for k in range(count_ops):
            part = jnp.concatenate(
                [grouped[per_row * r + cols * k : per_row * r + cols * (k + 1), :] for r in range(rows)], axis=0
            )
            hi, lo = split(part)
            term = nn(jnp.concatenate([hi, lo], axis=0), tt[k])
            total = term if total is None else total + term
        moved = jnp.where(lane < coeffs, total[:spheres] + total[spheres:], 0.0)
        if h == 1:
            hear(3)
            tell(4)
        result = apply_kinds(moved)
        return result

    once = couple(0)
    set_field(1, once)
    exchange(1)
    hear(1)
    tell(2)
    second = couple(1)
    state[2] = second
    base, once = state[0], state[1]

    def inner(a, b):
        return jnp.sum(jnp.sum(a * b, axis=0, keepdims=True), axis=1, keepdims=True)

    products = (
        inner(base, base), inner(base, once), inner(once, once),
        inner(base, second), inner(once, second), inner(second, second),
    )
    slot = iota((1, 128), 1)
    packed = jnp.zeros((1, 128), F32)
    for n, value in enumerate(products):
        packed = jnp.where(slot == n, value, packed)
    def all_sum(n, value, out, into, peers):
        out[...] = value
        for d, peer in enumerate(peers):
            pltpu.make_async_remote_copy(
                src_ref=out, dst_ref=into.at[d], send_sem=ar_send.at[n], recv_sem=ar_recv.at[n],
                device_id=peer, device_id_type=MESH,
            ).start()
        pltpu.make_async_copy(into, into, ar_recv.at[n]).wait()
        total = value
        for d in range(len(peers)):
            total = total + into[d]
        return total

    def far_first(n, inner):
        def hops(d):
            return min(d // inner, n // inner - d // inner) + min(d % inner, inner - d % inner)

        return sorted(range(1, n), key=lambda d: -hops(d))
    packed = all_sum(0, packed, one_out, one_in, [device(d, 0) for d in far_first(ngx, 2)])
    hear(4)
    packed = all_sum(1, packed, two_out, two_in, [device(0, d) for d in far_first(ngy, 8)])
    sums[...] = packed
    sent(0)
    sent(1)
    pltpu.make_async_copy(one_in, one_in, ar_send.at[0]).wait()
    pltpu.make_async_copy(two_in, two_in, ar_send.at[1]).wait()


def combine(state, sums, sol_ref, res_ref):
    rows, cols, coeffs = sol_ref.shape
    packed = sums[...]
    slot = iota((1, 128), 1)
    base, once, second = [state[n][:, :coeffs] for n in range(3)]

    def entry(n):
        return jnp.sum(jnp.where(slot == n, packed, 0.0), axis=1, keepdims=True)

    g00, g01, g11, g02, g12, g22 = [entry(n) for n in range(6)]
    gram = ((g00, g01, g02), (g01, g11, g12), (g02, g12, g22))

    def pair(a, b):
        total = None
        for i in range(3):
            for j in range(3):
                if a[i] is not None and b[j] is not None:
                    term = a[i] * b[j] * gram[i][j]
                    total = term if total is None else total + term
        return total

    beta2 = g00 + EPSILON
    beta = jnp.sqrt(beta2)
    ib = 1.0 / beta
    shift = (g01 + EPSILON) * ib * ib
    h11 = (g00 - g01) * ib * ib
    rest = (shift * ib, -ib, None)
    h21 = jnp.sqrt(jnp.maximum(pair(rest, rest), 0.0) + EPSILON)
    q = ib / h21
    v1 = (ib, None, None)
    v2 = (shift * q, -q, None)
    m2 = (shift * q, -(1.0 + shift) * q, q)
    h12 = pair(m2, v1)
    left = (m2[0] - h12 * ib, m2[1], m2[2])
    h22 = pair(left, v2)
    left = (left[0] - h22 * v2[0], left[1] - h22 * v2[1], left[2])
    h32 = jnp.sqrt(jnp.maximum(pair(left, left), 0.0) + EPSILON)
    aa = h11 * h11 + h21 * h21
    ab = h11 * h12 + h21 * h22
    bb = h12 * h12 + h22 * h22 + h32 * h32
    ra, rb = beta * h11, beta * h12
    determ = aa * bb - ab * ab
    y1 = (bb * ra - ab * rb) / determ
    y2 = (aa * rb - ab * ra) / determ
    s0 = y1 * ib + y2 * v2[0]
    s1 = y2 * v2[1]
    r0 = 1.0 - s0
    r1 = y1 * ib - y2 * m2[1]
    r2 = -y2 * q
    sol_ref[...] = (s0 * base + s1 * once).reshape(rows, cols, coeffs)
    res_ref[...] = (r0 * base + r1 * once + r2 * second).reshape(rows, cols, coeffs)


def solution(mesh):
    ngx, ngy = mesh.shape["gx"], mesh.shape["gy"]

    def body(incident, sphere_kinds, pair_codes, operators, pair_valid, translations, tmatrices):
        rows, cols, coeffs = incident.shape
        spheres = rows * cols
        count_ops, kinds_n = translations.shape[0], tmatrices.shape[0]
        vmem = pl.BlockSpec(memory_space=pltpu.VMEM)
        hbm = pl.BlockSpec(memory_space=pltpu.HBM)
        args = (incident, sphere_kinds, pair_codes, operators, pair_valid, translations, tmatrices)
        state, sums = pl.pallas_call(
            functools.partial(kernel, ngx, ngy),
            out_shape=(pltpu.VMEM((3, spheres, LANES), F32), pltpu.VMEM((1, 128), F32)),
            in_specs=[hbm] * 7,
            out_specs=(vmem, vmem),
            scratch_shapes=[pltpu.VMEM(arg.shape, arg.dtype) for arg in args]
            + [pltpu.VMEM(tmatrices.shape, BF16)] * 2
            + [pltpu.VMEM((kinds_n, LANES, LANES), BF16)] * 2
            + [
                pltpu.VMEM((kinds_n, 2 * spheres, LANES), BF16),
                pltpu.VMEM((count_ops, LANES, LANES), BF16),
                pltpu.VMEM((2, spheres * count_ops, 128), F32),
                pltpu.VMEM((spheres * count_ops, LANES), F32),
                pltpu.VMEM((2, 3 * spheres, LANES), F32),
                pltpu.VMEM((2, 96, LANES), F32),
                pltpu.VMEM((2, 2, 16, LANES), F32),
                pltpu.VMEM((3 * spheres + 96, LANES), BF16),
                pltpu.VMEM((3 * spheres + 96, LANES), BF16),
                pltpu.VMEM((1, 128), F32),
                pltpu.VMEM((ngx - 1, 1, 128), F32),
                pltpu.VMEM((1, 128), F32),
                pltpu.VMEM((ngy - 1, 1, 128), F32),
                pltpu.SemaphoreType.DMA((7,)),
                pltpu.SemaphoreType.DMA((2, len(PIECES))),
                pltpu.SemaphoreType.DMA((2, len(PIECES))),
                pltpu.SemaphoreType.DMA((2,)),
                pltpu.SemaphoreType.DMA((2,)),
                pltpu.SemaphoreType.REGULAR((2, 5)),
            ],
            compiler_params=pltpu.CompilerParams(collective_id=0, has_side_effects=True),
        )(*args)
        state, sums = [pltpu.with_memory_space_constraint(x, pltpu.VMEM) for x in (state, sums)]
        return pl.pallas_call(
            combine,
            out_shape=(jax.ShapeDtypeStruct(incident.shape, F32),) * 2,
            in_specs=[vmem] * 2,
            out_specs=(vmem, vmem),
        )(state, sums)

    here, line, table = P("gx", "gy", None), P("gx", "gy"), P()
    return jax.shard_map(
        body, mesh=mesh, in_specs=(here, line, here, here, here, table, table), out_specs=(here, here), check_vma=False
    )
```

```python
import functools

import jax
import jax.numpy as jnp
from jax import lax
from jax.experimental import pallas as pl
from jax.experimental.pallas import tpu as pltpu
from jax.sharding import PartitionSpec as P

MESH = pl.DeviceIdType.MESH
HALO = 4
STRIDE = 2 * HALO + 1
LANES = 256
EPSILON = 1e-06
F32, BF16 = jnp.float32, jnp.bfloat16

PIECES = (
    (1, 1, 2, 0, 16),
    (-1, 1, 2, 32, 16),
    (1, -1, 1, 48, 16),
    (-1, -1, 1, 80, 16),
    (0, 1, 2, 16, 16),
    (0, -1, 1, 64, 16),
    (1, 0, 0, 0, 64),
    (-1, 0, 0, 128, 64),
)


def nt(a, b):
    return lax.dot_general(a, b, (((1,), (1,)), ((), ())), preferred_element_type=F32)


def nn(a, b):
    return lax.dot_general(a, b, (((1,), (0,)), ((), ())), preferred_element_type=F32)


def split(x):
    hi = x.astype(BF16)
    return hi, (x - hi.astype(F32)).astype(BF16)


def iota(shape, dim):
    return lax.broadcasted_iota(jnp.int32, shape, dim)


def spread(n):
    steps, d = [], 1
    while d < n - 1:
        steps.append(d)
        d *= 2
    return steps


def kernel(
    ngx, ngy, inc_hbm, kinds_hbm, codes_hbm, ops_hbm, valid_hbm, trans_hbm, tmat_hbm,
    state, sums,
    inc_ref, kinds_ref, codes_ref, ops_ref, valid_ref, trans_v, tmat_v,
    tmhi, tmlo, tmhi_t, tmlo_t, masks, tt, counts, grouped, mid, side, edge, vhi, vlo,
    one_out, one_in, two_out, two_in,
    load_sem, halo_send, halo_recv, ar_send, ar_recv, spread_sem,
):
    gx, gy = lax.axis_index("gx"), lax.axis_index("gy")
    rows, cols, coeffs = inc_ref.shape
    spheres = rows * cols
    slots = codes_ref.shape[2]
    count_ops, kinds_n = trans_v.shape[0], tmat_v.shape[0]

    def device(dx, dy):
        return (lax.rem(gx + (dx + ngx), ngx), lax.rem(gy + (dy + ngy), ngy))

    def inside_tests(dx, dy):
        tests = []
        for at, n, d in ((gx, ngx, dx), (gy, ngy, dy)):
            if d > 0:
                tests.append(at < n - d)
            elif d < 0:
                tests.append(at >= -d)
        return tests

    def when(dx, dy):
        return pl.when(functools.reduce(jnp.logical_and, inside_tests(dx, dy)))

    def count_at(at, size, d):
        return (at >= d).astype(jnp.int32) + (at < size - d).astype(jnp.int32)

    def there(dx, dy):
        return (gx + dx, gy + dy)
    barrier = pltpu.get_barrier_semaphore()
    for dx, dy, _, _, _ in PIECES:

        @when(dx, dy)
        def _():
            pl.semaphore_signal(barrier, inc=1, device_id=there(dx, dy), device_id_type=MESH)

    loads = []
    for n, (src, dst) in enumerate((
        (tmat_hbm, tmat_v), (inc_hbm, inc_ref), (kinds_hbm, kinds_ref), (codes_hbm, codes_ref),
        (ops_hbm, ops_ref), (valid_hbm, valid_ref), (trans_hbm, trans_v),
    )):
        loads.append(pltpu.make_async_copy(src, dst, load_sem.at[n]))
    for n in range(3):
        loads[n].start()

    rounds = [[(0, d) for d in spread(ngy)], [(d, 0) for d in spread(ngx)]]

    def tell(n):
        for axis, steps in enumerate(rounds):
            if n < len(steps):
                dx, dy = steps[n]
                for sign in (1, -1):

                    @when(sign * dx, sign * dy)
                    def _():
                        pl.semaphore_signal(
                            spread_sem.at[axis, n], inc=1, device_id=there(sign * dx, sign * dy), device_id_type=MESH
                        )


    def hear(n):
        for axis, steps in enumerate(rounds):
            if n < len(steps):
                at, size = ((gy, ngy), (gx, ngx))[axis]
                pl.semaphore_wait(spread_sem.at[axis, n], count_at(at, size, sum(steps[n])))
    for n in range(3):
        loads[n].wait()
    for n in range(3, 7):
        loads[n].start()
    lane = iota((spheres, LANES), 1)
    eye = iota((cols, cols), 0) == iota((cols, cols), 1)
    kind_col = jnp.concatenate(
        [
            jnp.sum(
                jnp.where(eye, jnp.broadcast_to(kinds_ref[r : r + 1, :], (cols, cols)), 0).astype(F32),
                axis=1, keepdims=True,
            )
            for r in range(rows)
        ],
        axis=0,
    )

    def source_of(u):
        total = None
        for p in range(kinds_n):
            hi, lo = split(jnp.where(kind_col == p, u, 0.0))
            term = nt(hi, tmhi[p]) + nt(lo, tmhi[p]) + nt(hi, tmlo[p])
            total = term if total is None else total + term
        return total

    def apply_kinds(u):
        hi, lo = split(u)
        both = jnp.concatenate([hi, lo], axis=0)
        wide, fine = None, None
        for p in range(kinds_n):
            chosen = both * masks[p]
            term, more = nn(chosen, tmhi_t[p]), nn(chosen[:spheres], tmlo_t[p])
            wide, fine = (term, more) if wide is None else (wide + term, fine + more)
        return jnp.where(lane < coeffs, wide[:spheres] + wide[spheres:] + fine, 0.0)

    def set_field(h, u):
        mid[h, spheres : 2 * spheres, :] = u
        state[h] = u
        for r in range(rows):
            for e, c in ((0, 0), (1, cols - HALO)):
                edge[h, e, HALO * r : HALO * (r + 1), :] = mid[
                    h, spheres + cols * r + c : spheres + cols * r + c + HALO, :
                ]

    def pieces(h):
        for n, (dx, dy, source, first, count) in enumerate(PIECES):
            if source == 0:
                src, dst = mid.at[h, pl.ds(spheres, spheres)], mid.at[h, pl.ds(first, count)]
            else:
                src, dst = edge.at[h, source - 1], side.at[h, pl.ds(first, count)]
            copy = pltpu.make_async_remote_copy(
                src_ref=src, dst_ref=dst, send_sem=halo_send.at[h, n], recv_sem=halo_recv.at[h, n],
                device_id=there(dx, dy), device_id_type=MESH,
            )
            yield dx, dy, copy

    def exchange(h):
        for dx, dy, copy in pieces(h):
            when(dx, dy)(copy.start)

    def arrive(h):
        for dx, dy, copy in pieces(h):
            when(-dx, -dy)(copy.wait_recv)

    def sent(h):
        for dx, dy, copy in pieces(h):
            when(dx, dy)(copy.wait_send)

    for dx, dy, source, first, count in PIECES:

        @pl.when(jnp.logical_not(functools.reduce(jnp.logical_and, inside_tests(-dx, -dy))))
        def _():
            for h in range(2):
                (mid if source == 0 else side)[h, first : first + count, :] = jnp.zeros((count, LANES), F32)

    for p in range(kinds_n):
        hi, lo = split(tmat_v[p])
        tmhi[p] = hi
        tmlo[p] = lo
    state[0] = jnp.zeros((spheres, LANES), F32)
    state[0, :, :coeffs] = source_of(inc_ref[...].reshape(spheres, coeffs))
    set_field(0, state[0])
    near_x, near_y = count_at(gx, ngx, 1), count_at(gy, ngy, 1)
    pl.semaphore_wait(barrier, (near_x + 1) * (near_y + 1) - 1)
    exchange(0)
    tell(0)
    for n in range(3, 6):
        loads[n].wait()
    codes = codes_ref[...].reshape(spheres, slots)
    sphere = iota((spheres, slots), 0)
    row, col = sphere >> 4, sphere & 15
    step_x = (codes * 57) >> 9
    ext_x = row + step_x
    ext_y = col + codes - STRIDE * step_x
    target = jnp.where(
        ext_y < HALO,
        144 + HALO * ext_x + ext_y,
        jnp.where(ext_y < HALO + cols, cols * step_x + ext_y - HALO, 172 + HALO * ext_x + ext_y),
    )
    at_x = gx * rows + ext_x - HALO
    at_y = gy * cols + ext_y - HALO
    inside = (at_x >= 0) & (at_x < ngx * rows) & (at_y >= 0) & (at_y < ngy * cols)
    inside = inside & (valid_ref[...].reshape(spheres, slots) == 1)
    key = jnp.where(inside, row * count_ops + ops_ref[...].reshape(spheres, slots), -1)
    target = jnp.concatenate([target[cols * r : cols * (r + 1)] for r in range(rows)], axis=1)
    key = jnp.concatenate([key[cols * r : cols * (r + 1)] for r in range(rows)], axis=1)
    for c in range(cols):
        left = (iota((rows * count_ops, LANES), 0) == key[c : c + 1, :]).astype(F32).astype(BF16)
        right = (iota((LANES, LANES), 0) == target[c : c + 1, :]).astype(F32).astype(BF16)
        tally = nt(left, right)
        for r in range(rows):
            piece = tally[count_ops * r : count_ops * (r + 1)]
            for half in range(2):
                counts[half, pl.ds(r * cols * count_ops + c, count_ops, stride=cols), :] = piece[
                    :, 128 * half : 128 * (half + 1)
                ]

    loads[6].wait()
    unit = (iota((LANES, coeffs), 0) == iota((LANES, coeffs), 1)).astype(F32).astype(BF16)
    for k in range(count_ops):
        tt[k, :, :coeffs] = nt(unit, trans_v[k]).astype(BF16)
    for p in range(kinds_n):
        tmhi_t[p, :, :coeffs] = nt(unit, tmhi[p]).astype(BF16)
        tmlo_t[p, :, :coeffs] = nt(unit, tmlo[p]).astype(BF16)
        mask = jnp.where(jnp.broadcast_to(kind_col, (spheres, LANES)) == p, 1.0, 0.0)
        masks[p] = jnp.concatenate([mask, mask], axis=0).astype(BF16)
    hear(0)
    tell(1)
    def couple(h):
        arrive(h)
        if h == 0:
            hear(1)
            tell(2)
        hi, lo = split(mid[h])
        vhi[: 3 * spheres], vlo[: 3 * spheres] = hi, lo
        hi, lo = split(side[h])
        vhi[3 * spheres :], vlo[3 * spheres :] = hi, lo
        tail = jnp.zeros((16, LANES), BF16)
        per_row = cols * count_ops
        for r in range(rows):
            table = jnp.concatenate(
                [counts[half, per_row * r : per_row * (r + 1), :].astype(BF16) for half in range(2)], axis=1
            )
            near = [
                jnp.concatenate([v[cols * r : cols * (r + STRIDE)], v[3 * spheres :], tail], axis=0)
                for v in (vhi, vlo)
            ]
            grouped[per_row * r : per_row * (r + 1), :] = nn(table, near[0]) + nn(table, near[1])
        total = None
        for k in range(count_ops):
            part = jnp.concatenate(
                [grouped[per_row * r + cols * k : per_row * r + cols * (k + 1), :] for r in range(rows)], axis=0
            )
            hi, lo = split(part)
            term = nn(jnp.concatenate([hi, lo], axis=0), tt[k])
            total = term if total is None else total + term
        moved = jnp.where(lane < coeffs, total[:spheres] + total[spheres:], 0.0)
        result = apply_kinds(moved)
        return result

    once = couple(0)
    set_field(1, once)
    exchange(1)
    hear(2)
    tell(3)
    second = couple(1)
    state[2] = second
    base, once = state[0], state[1]

    def inner(a, b):
        return jnp.sum(jnp.sum(a * b, axis=0, keepdims=True), axis=1, keepdims=True)

    products = (
        inner(base, base), inner(base, once), inner(once, once),
        inner(base, second), inner(once, second), inner(second, second),
    )
    slot = iota((1, 128), 1)
    packed = jnp.zeros((1, 128), F32)
    for n, value in enumerate(products):
        packed = jnp.where(slot == n, value, packed)
    def all_sum(n, value, out, into, peers):
        out[...] = value
        for d, peer in enumerate(peers):
            pltpu.make_async_remote_copy(
                src_ref=out, dst_ref=into.at[d], send_sem=ar_send.at[n], recv_sem=ar_recv.at[n],
                device_id=peer, device_id_type=MESH,
            ).start()
        pltpu.make_async_copy(into, into, ar_recv.at[n]).wait()
        total = value
        for d in range(len(peers)):
            total = total + into[d]
        return total

    def far_first(n, inner):
        def hops(d):
            return min(d // inner, n // inner - d // inner) + min(d % inner, inner - d % inner)

        return sorted(range(1, n), key=lambda d: -hops(d))
    hear(3)
    tell(4)
    packed = all_sum(0, packed, one_out, one_in, [device(d, 0) for d in far_first(ngx, 2)])
    hear(4)
    packed = all_sum(1, packed, two_out, two_in, [device(0, d) for d in far_first(ngy, 8)])
    sums[...] = packed
    sent(0)
    sent(1)
    pltpu.make_async_copy(one_in, one_in, ar_send.at[0]).wait()
    pltpu.make_async_copy(two_in, two_in, ar_send.at[1]).wait()


def combine(state, sums, sol_ref, res_ref):
    rows, cols, coeffs = sol_ref.shape
    packed = sums[...]
    slot = iota((1, 128), 1)
    base, once, second = [state[n][:, :coeffs] for n in range(3)]

    def entry(n):
        return jnp.sum(jnp.where(slot == n, packed, 0.0), axis=1, keepdims=True)

    g00, g01, g11, g02, g12, g22 = [entry(n) for n in range(6)]
    gram = ((g00, g01, g02), (g01, g11, g12), (g02, g12, g22))

    def pair(a, b):
        total = None
        for i in range(3):
            for j in range(3):
                if a[i] is not None and b[j] is not None:
                    term = a[i] * b[j] * gram[i][j]
                    total = term if total is None else total + term
        return total

    beta2 = g00 + EPSILON
    beta = jnp.sqrt(beta2)
    ib = 1.0 / beta
    shift = (g01 + EPSILON) * ib * ib
    h11 = (g00 - g01) * ib * ib
    rest = (shift * ib, -ib, None)
    h21 = jnp.sqrt(jnp.maximum(pair(rest, rest), 0.0) + EPSILON)
    q = ib / h21
    v1 = (ib, None, None)
    v2 = (shift * q, -q, None)
    m2 = (shift * q, -(1.0 + shift) * q, q)
    h12 = pair(m2, v1)
    left = (m2[0] - h12 * ib, m2[1], m2[2])
    h22 = pair(left, v2)
    left = (left[0] - h22 * v2[0], left[1] - h22 * v2[1], left[2])
    h32 = jnp.sqrt(jnp.maximum(pair(left, left), 0.0) + EPSILON)
    aa = h11 * h11 + h21 * h21
    ab = h11 * h12 + h21 * h22
    bb = h12 * h12 + h22 * h22 + h32 * h32
    ra, rb = beta * h11, beta * h12
    determ = aa * bb - ab * ab
    y1 = (bb * ra - ab * rb) / determ
    y2 = (aa * rb - ab * ra) / determ
    s0 = y1 * ib + y2 * v2[0]
    s1 = y2 * v2[1]
    r0 = 1.0 - s0
    r1 = y1 * ib - y2 * m2[1]
    r2 = -y2 * q
    sol_ref[...] = (s0 * base + s1 * once).reshape(rows, cols, coeffs)
    res_ref[...] = (r0 * base + r1 * once + r2 * second).reshape(rows, cols, coeffs)


def solution(mesh):
    ngx, ngy = mesh.shape["gx"], mesh.shape["gy"]

    def body(incident, sphere_kinds, pair_codes, operators, pair_valid, translations, tmatrices):
        rows, cols, coeffs = incident.shape
        spheres = rows * cols
        count_ops, kinds_n = translations.shape[0], tmatrices.shape[0]
        vmem = pl.BlockSpec(memory_space=pltpu.VMEM)
        hbm = pl.BlockSpec(memory_space=pltpu.HBM)
        args = (incident, sphere_kinds, pair_codes, operators, pair_valid, translations, tmatrices)
        state, sums = pl.pallas_call(
            functools.partial(kernel, ngx, ngy),
            out_shape=(pltpu.VMEM((3, spheres, LANES), F32), pltpu.VMEM((1, 128), F32)),
            in_specs=[hbm] * 7,
            out_specs=(vmem, vmem),
            scratch_shapes=[pltpu.VMEM(arg.shape, arg.dtype) for arg in args]
            + [pltpu.VMEM(tmatrices.shape, BF16)] * 2
            + [pltpu.VMEM((kinds_n, LANES, LANES), BF16)] * 2
            + [
                pltpu.VMEM((kinds_n, 2 * spheres, LANES), BF16),
                pltpu.VMEM((count_ops, LANES, LANES), BF16),
                pltpu.VMEM((2, spheres * count_ops, 128), F32),
                pltpu.VMEM((spheres * count_ops, LANES), F32),
                pltpu.VMEM((2, 3 * spheres, LANES), F32),
                pltpu.VMEM((2, 96, LANES), F32),
                pltpu.VMEM((2, 2, 16, LANES), F32),
                pltpu.VMEM((3 * spheres + 96, LANES), BF16),
                pltpu.VMEM((3 * spheres + 96, LANES), BF16),
                pltpu.VMEM((1, 128), F32),
                pltpu.VMEM((ngx - 1, 1, 128), F32),
                pltpu.VMEM((1, 128), F32),
                pltpu.VMEM((ngy - 1, 1, 128), F32),
                pltpu.SemaphoreType.DMA((7,)),
                pltpu.SemaphoreType.DMA((2, len(PIECES))),
                pltpu.SemaphoreType.DMA((2, len(PIECES))),
                pltpu.SemaphoreType.DMA((2,)),
                pltpu.SemaphoreType.DMA((2,)),
                pltpu.SemaphoreType.REGULAR((2, 5)),
            ],
            compiler_params=pltpu.CompilerParams(collective_id=0, has_side_effects=True),
        )(*args)
        state, sums = [pltpu.with_memory_space_constraint(x, pltpu.VMEM) for x in (state, sums)]
        return pl.pallas_call(
            combine,
            out_shape=(jax.ShapeDtypeStruct(incident.shape, F32),) * 2,
            in_specs=[vmem] * 2,
            out_specs=(vmem, vmem),
        )(state, sums)

    here, line, table = P("gx", "gy", None), P("gx", "gy"), P()
    return jax.shard_map(
        body, mesh=mesh, in_specs=(here, line, here, here, here, table, table), out_specs=(here, here), check_vma=False
    )
```

```python
import functools

import jax
import jax.numpy as jnp
from jax import lax
from jax.experimental import pallas as pl
from jax.experimental.pallas import tpu as pltpu
from jax.sharding import PartitionSpec as P

MESH = pl.DeviceIdType.MESH
HALO = 4
STRIDE = 2 * HALO + 1
LANES = 256
EPSILON = 1e-06
F32, BF16 = jnp.float32, jnp.bfloat16

PIECES = (
    (1, 1, 2, 0, 16),
    (-1, 1, 2, 32, 16),
    (1, -1, 1, 48, 16),
    (-1, -1, 1, 80, 16),
    (0, 1, 2, 16, 16),
    (0, -1, 1, 64, 16),
    (1, 0, 0, 0, 64),
    (-1, 0, 0, 128, 64),
)


def nt(a, b):
    return lax.dot_general(a, b, (((1,), (1,)), ((), ())), preferred_element_type=F32)


def nn(a, b):
    return lax.dot_general(a, b, (((1,), (0,)), ((), ())), preferred_element_type=F32)


def split(x):
    hi = x.astype(BF16)
    return hi, (x - hi.astype(F32)).astype(BF16)


def iota(shape, dim):
    return lax.broadcasted_iota(jnp.int32, shape, dim)


def spread(n):
    steps, d = [], 1
    while d < n - 1:
        steps.append(d)
        d *= 2
    return steps


def kernel(
    ngx, ngy, inc_hbm, kinds_hbm, codes_hbm, ops_hbm, valid_hbm, trans_hbm, tmat_hbm,
    state, sums,
    inc_ref, kinds_ref, codes_ref, ops_ref, valid_ref, trans_v, tmat_v,
    tmhi, tmlo, tmhi_t, tmlo_t, masks, tt, counts, grouped, mid, side, edge, vhi, vlo,
    one_out, one_in, two_out, two_in,
    load_sem, halo_send, halo_recv, ar_send, ar_recv, spread_sem,
):
    gx, gy = lax.axis_index("gx"), lax.axis_index("gy")
    rows, cols, coeffs = inc_ref.shape
    spheres = rows * cols
    slots = codes_ref.shape[2]
    count_ops, kinds_n = trans_v.shape[0], tmat_v.shape[0]

    def device(dx, dy):
        return (lax.rem(gx + (dx + ngx), ngx), lax.rem(gy + (dy + ngy), ngy))

    def inside_tests(dx, dy):
        tests = []
        for at, n, d in ((gx, ngx, dx), (gy, ngy, dy)):
            if d > 0:
                tests.append(at < n - d)
            elif d < 0:
                tests.append(at >= -d)
        return tests

    def when(dx, dy):
        return pl.when(functools.reduce(jnp.logical_and, inside_tests(dx, dy)))

    def count_at(at, size, d):
        return (at >= d).astype(jnp.int32) + (at < size - d).astype(jnp.int32)

    def there(dx, dy):
        return (gx + dx, gy + dy)
    barrier = pltpu.get_barrier_semaphore()
    for dx, dy, _, _, _ in PIECES:

        @when(dx, dy)
        def _():
            pl.semaphore_signal(barrier, inc=1, device_id=there(dx, dy), device_id_type=MESH)

    loads = []
    for n, (src, dst) in enumerate((
        (tmat_hbm, tmat_v), (inc_hbm, inc_ref), (kinds_hbm, kinds_ref), (codes_hbm, codes_ref),
        (ops_hbm, ops_ref), (valid_hbm, valid_ref), (trans_hbm, trans_v),
    )):
        loads.append(pltpu.make_async_copy(src, dst, load_sem.at[n]))
    for n in range(3):
        loads[n].start()

    rounds = [[(0, d) for d in spread(ngy)], [(d, 0) for d in spread(ngx)]]

    def tell(n):
        for axis, steps in enumerate(rounds):
            if n < len(steps):
                dx, dy = steps[n]
                for sign in (1, -1):

                    @when(sign * dx, sign * dy)
                    def _():
                        pl.semaphore_signal(
                            spread_sem.at[axis, n], inc=1, device_id=there(sign * dx, sign * dy), device_id_type=MESH
                        )


    def hear(n):
        for axis, steps in enumerate(rounds):
            if n < len(steps):
                at, size = ((gy, ngy), (gx, ngx))[axis]
                pl.semaphore_wait(spread_sem.at[axis, n], count_at(at, size, sum(steps[n])))
    for n in range(3):
        loads[n].wait()
    for n in range(3, 7):
        loads[n].start()
    lane = iota((spheres, LANES), 1)
    eye = iota((cols, cols), 0) == iota((cols, cols), 1)
    kind_col = jnp.concatenate(
        [
            jnp.sum(
                jnp.where(eye, jnp.broadcast_to(kinds_ref[r : r + 1, :], (cols, cols)), 0).astype(F32),
                axis=1, keepdims=True,
            )
            for r in range(rows)
        ],
        axis=0,
    )

    def source_of(u):
        total = None
        for p in range(kinds_n):
            hi, lo = split(jnp.where(kind_col == p, u, 0.0))
            term = nt(hi, tmhi[p]) + nt(lo, tmhi[p]) + nt(hi, tmlo[p])
            total = term if total is None else total + term
        return total

    def apply_kinds(u):
        hi, lo = split(u)
        both = jnp.concatenate([hi, lo], axis=0)
        wide, fine = None, None
        for p in range(kinds_n):
            chosen = both * masks[p]
            term, more = nn(chosen, tmhi_t[p]), nn(chosen[:spheres], tmlo_t[p])
            wide, fine = (term, more) if wide is None else (wide + term, fine + more)
        return jnp.where(lane < coeffs, wide[:spheres] + wide[spheres:] + fine, 0.0)

    def set_field(h, u):
        mid[h, spheres : 2 * spheres, :] = u
        state[h] = u
        for r in range(rows):
            for e, c in ((0, 0), (1, cols - HALO)):
                edge[h, e, HALO * r : HALO * (r + 1), :] = mid[
                    h, spheres + cols * r + c : spheres + cols * r + c + HALO, :
                ]

    def pieces(h):
        for n, (dx, dy, source, first, count) in enumerate(PIECES):
            if source == 0:
                src, dst = mid.at[h, pl.ds(spheres, spheres)], mid.at[h, pl.ds(first, count)]
            else:
                src, dst = edge.at[h, source - 1], side.at[h, pl.ds(first, count)]
            copy = pltpu.make_async_remote_copy(
                src_ref=src, dst_ref=dst, send_sem=halo_send.at[h, n], recv_sem=halo_recv.at[h, n],
                device_id=there(dx, dy), device_id_type=MESH,
            )
            yield dx, dy, copy

    def exchange(h):
        for dx, dy, copy in pieces(h):
            when(dx, dy)(copy.start)

    def arrive(h):
        for dx, dy, copy in pieces(h):
            when(-dx, -dy)(copy.wait_recv)

    def sent(h):
        for dx, dy, copy in pieces(h):
            when(dx, dy)(copy.wait_send)

    for dx, dy, source, first, count in PIECES:

        @pl.when(jnp.logical_not(functools.reduce(jnp.logical_and, inside_tests(-dx, -dy))))
        def _():
            for h in range(2):
                (mid if source == 0 else side)[h, first : first + count, :] = jnp.zeros((count, LANES), F32)

    for p in range(kinds_n):
        hi, lo = split(tmat_v[p])
        tmhi[p] = hi
        tmlo[p] = lo
    state[0] = jnp.zeros((spheres, LANES), F32)
    state[0, :, :coeffs] = source_of(inc_ref[...].reshape(spheres, coeffs))
    set_field(0, state[0])
    near_x, near_y = count_at(gx, ngx, 1), count_at(gy, ngy, 1)
    pl.semaphore_wait(barrier, (near_x + 1) * (near_y + 1) - 1)
    exchange(0)
    tell(0)
    for n in range(3, 6):
        loads[n].wait()
    codes = codes_ref[...].reshape(spheres, slots)
    sphere = iota((spheres, slots), 0)
    row, col = sphere >> 4, sphere & 15
    step_x = (codes * 57) >> 9
    ext_x = row + step_x
    ext_y = col + codes - STRIDE * step_x
    target = jnp.where(
        ext_y < HALO,
        144 + HALO * ext_x + ext_y,
        jnp.where(ext_y < HALO + cols, cols * step_x + ext_y - HALO, 172 + HALO * ext_x + ext_y),
    )
    at_x = gx * rows + ext_x - HALO
    at_y = gy * cols + ext_y - HALO
    inside = (at_x >= 0) & (at_x < ngx * rows) & (at_y >= 0) & (at_y < ngy * cols)
    inside = inside & (valid_ref[...].reshape(spheres, slots) == 1)
    key = jnp.where(inside, row * count_ops + ops_ref[...].reshape(spheres, slots), -1)
    target = jnp.concatenate([target[cols * r : cols * (r + 1)] for r in range(rows)], axis=1)
    key = jnp.concatenate([key[cols * r : cols * (r + 1)] for r in range(rows)], axis=1)
    for c in range(cols):
        left = (iota((rows * count_ops, LANES), 0) == key[c : c + 1, :]).astype(F32).astype(BF16)
        right = (iota((LANES, LANES), 0) == target[c : c + 1, :]).astype(F32).astype(BF16)
        tally = nt(left, right)
        for r in range(rows):
            piece = tally[count_ops * r : count_ops * (r + 1)]
            for half in range(2):
                counts[half, pl.ds(r * cols * count_ops + c, count_ops, stride=cols), :] = piece[
                    :, 128 * half : 128 * (half + 1)
                ]

    loads[6].wait()
    hear(0)
    tell(1)
    unit = (iota((LANES, coeffs), 0) == iota((LANES, coeffs), 1)).astype(F32).astype(BF16)
    for k in range(count_ops):
        tt[k, :, :coeffs] = nt(unit, trans_v[k]).astype(BF16)
    for p in range(kinds_n):
        tmhi_t[p, :, :coeffs] = nt(unit, tmhi[p]).astype(BF16)
        tmlo_t[p, :, :coeffs] = nt(unit, tmlo[p]).astype(BF16)
        mask = jnp.where(jnp.broadcast_to(kind_col, (spheres, LANES)) == p, 1.0, 0.0)
        masks[p] = jnp.concatenate([mask, mask], axis=0).astype(BF16)
    def couple(h):
        arrive(h)
        if h == 0:
            hear(1)
            tell(2)
        hi, lo = split(mid[h])
        vhi[: 3 * spheres], vlo[: 3 * spheres] = hi, lo
        hi, lo = split(side[h])
        vhi[3 * spheres :], vlo[3 * spheres :] = hi, lo
        tail = jnp.zeros((16, LANES), BF16)
        per_row = cols * count_ops
        for r in range(rows):
            table = jnp.concatenate(
                [counts[half, per_row * r : per_row * (r + 1), :].astype(BF16) for half in range(2)], axis=1
            )
            near = [
                jnp.concatenate([v[cols * r : cols * (r + STRIDE)], v[3 * spheres :], tail], axis=0)
                for v in (vhi, vlo)
            ]
            grouped[per_row * r : per_row * (r + 1), :] = nn(table, near[0]) + nn(table, near[1])
        total = None
        for k in range(count_ops):
            part = jnp.concatenate(
                [grouped[per_row * r + cols * k : per_row * r + cols * (k + 1), :] for r in range(rows)], axis=0
            )
            hi, lo = split(part)
            term = nn(jnp.concatenate([hi, lo], axis=0), tt[k])
            total = term if total is None else total + term
        moved = jnp.where(lane < coeffs, total[:spheres] + total[spheres:], 0.0)
        result = apply_kinds(moved)
        return result

    once = couple(0)
    set_field(1, once)
    exchange(1)
    hear(2)
    tell(3)
    second = couple(1)
    state[2] = second
    base, once = state[0], state[1]

    def inner(a, b):
        return jnp.sum(jnp.sum(a * b, axis=0, keepdims=True), axis=1, keepdims=True)

    products = (
        inner(base, base), inner(base, once), inner(once, once),
        inner(base, second), inner(once, second), inner(second, second),
    )
    slot = iota((1, 128), 1)
    packed = jnp.zeros((1, 128), F32)
    for n, value in enumerate(products):
        packed = jnp.where(slot == n, value, packed)
    def all_sum(n, value, out, into, peers):
        out[...] = value
        for d, peer in enumerate(peers):
            pltpu.make_async_remote_copy(
                src_ref=out, dst_ref=into.at[d], send_sem=ar_send.at[n], recv_sem=ar_recv.at[n],
                device_id=peer, device_id_type=MESH,
            ).start()
        pltpu.make_async_copy(into, into, ar_recv.at[n]).wait()
        total = value
        for d in range(len(peers)):
            total = total + into[d]
        return total

    def far_first(n, inner):
        def hops(d):
            return min(d // inner, n // inner - d // inner) + min(d % inner, inner - d % inner)

        return sorted(range(1, n), key=lambda d: -hops(d))
    hear(3)
    tell(4)
    packed = all_sum(0, packed, one_out, one_in, [device(d, 0) for d in far_first(ngx, 2)])
    hear(4)
    packed = all_sum(1, packed, two_out, two_in, [device(0, d) for d in far_first(ngy, 8)])
    sums[...] = packed
    sent(0)
    sent(1)
    pltpu.make_async_copy(one_in, one_in, ar_send.at[0]).wait()
    pltpu.make_async_copy(two_in, two_in, ar_send.at[1]).wait()


def combine(state, sums, sol_ref, res_ref):
    rows, cols, coeffs = sol_ref.shape
    packed = sums[...]
    slot = iota((1, 128), 1)
    base, once, second = [state[n][:, :coeffs] for n in range(3)]

    def entry(n):
        return jnp.sum(jnp.where(slot == n, packed, 0.0), axis=1, keepdims=True)

    g00, g01, g11, g02, g12, g22 = [entry(n) for n in range(6)]
    gram = ((g00, g01, g02), (g01, g11, g12), (g02, g12, g22))

    def pair(a, b):
        total = None
        for i in range(3):
            for j in range(3):
                if a[i] is not None and b[j] is not None:
                    term = a[i] * b[j] * gram[i][j]
                    total = term if total is None else total + term
        return total

    beta2 = g00 + EPSILON
    beta = jnp.sqrt(beta2)
    ib = 1.0 / beta
    shift = (g01 + EPSILON) * ib * ib
    h11 = (g00 - g01) * ib * ib
    rest = (shift * ib, -ib, None)
    h21 = jnp.sqrt(jnp.maximum(pair(rest, rest), 0.0) + EPSILON)
    q = ib / h21
    v1 = (ib, None, None)
    v2 = (shift * q, -q, None)
    m2 = (shift * q, -(1.0 + shift) * q, q)
    h12 = pair(m2, v1)
    left = (m2[0] - h12 * ib, m2[1], m2[2])
    h22 = pair(left, v2)
    left = (left[0] - h22 * v2[0], left[1] - h22 * v2[1], left[2])
    h32 = jnp.sqrt(jnp.maximum(pair(left, left), 0.0) + EPSILON)
    aa = h11 * h11 + h21 * h21
    ab = h11 * h12 + h21 * h22
    bb = h12 * h12 + h22 * h22 + h32 * h32
    ra, rb = beta * h11, beta * h12
    determ = aa * bb - ab * ab
    y1 = (bb * ra - ab * rb) / determ
    y2 = (aa * rb - ab * ra) / determ
    s0 = y1 * ib + y2 * v2[0]
    s1 = y2 * v2[1]
    r0 = 1.0 - s0
    r1 = y1 * ib - y2 * m2[1]
    r2 = -y2 * q
    sol_ref[...] = (s0 * base + s1 * once).reshape(rows, cols, coeffs)
    res_ref[...] = (r0 * base + r1 * once + r2 * second).reshape(rows, cols, coeffs)


def solution(mesh):
    ngx, ngy = mesh.shape["gx"], mesh.shape["gy"]

    def body(incident, sphere_kinds, pair_codes, operators, pair_valid, translations, tmatrices):
        rows, cols, coeffs = incident.shape
        spheres = rows * cols
        count_ops, kinds_n = translations.shape[0], tmatrices.shape[0]
        vmem = pl.BlockSpec(memory_space=pltpu.VMEM)
        hbm = pl.BlockSpec(memory_space=pltpu.HBM)
        args = (incident, sphere_kinds, pair_codes, operators, pair_valid, translations, tmatrices)
        state, sums = pl.pallas_call(
            functools.partial(kernel, ngx, ngy),
            out_shape=(pltpu.VMEM((3, spheres, LANES), F32), pltpu.VMEM((1, 128), F32)),
            in_specs=[hbm] * 7,
            out_specs=(vmem, vmem),
            scratch_shapes=[pltpu.VMEM(arg.shape, arg.dtype) for arg in args]
            + [pltpu.VMEM(tmatrices.shape, BF16)] * 2
            + [pltpu.VMEM((kinds_n, LANES, LANES), BF16)] * 2
            + [
                pltpu.VMEM((kinds_n, 2 * spheres, LANES), BF16),
                pltpu.VMEM((count_ops, LANES, LANES), BF16),
                pltpu.VMEM((2, spheres * count_ops, 128), F32),
                pltpu.VMEM((spheres * count_ops, LANES), F32),
                pltpu.VMEM((2, 3 * spheres, LANES), F32),
                pltpu.VMEM((2, 96, LANES), F32),
                pltpu.VMEM((2, 2, 16, LANES), F32),
                pltpu.VMEM((3 * spheres + 96, LANES), BF16),
                pltpu.VMEM((3 * spheres + 96, LANES), BF16),
                pltpu.VMEM((1, 128), F32),
                pltpu.VMEM((ngx - 1, 1, 128), F32),
                pltpu.VMEM((1, 128), F32),
                pltpu.VMEM((ngy - 1, 1, 128), F32),
                pltpu.SemaphoreType.DMA((7,)),
                pltpu.SemaphoreType.DMA((2, len(PIECES))),
                pltpu.SemaphoreType.DMA((2, len(PIECES))),
                pltpu.SemaphoreType.DMA((2,)),
                pltpu.SemaphoreType.DMA((2,)),
                pltpu.SemaphoreType.REGULAR((2, 5)),
            ],
            compiler_params=pltpu.CompilerParams(collective_id=0, has_side_effects=True),
        )(*args)
        state, sums = [pltpu.with_memory_space_constraint(x, pltpu.VMEM) for x in (state, sums)]
        return pl.pallas_call(
            combine,
            out_shape=(jax.ShapeDtypeStruct(incident.shape, F32),) * 2,
            in_specs=[vmem] * 2,
            out_specs=(vmem, vmem),
        )(state, sums)

    here, line, table = P("gx", "gy", None), P("gx", "gy"), P()
    return jax.shard_map(
        body, mesh=mesh, in_specs=(here, line, here, here, here, table, table), out_specs=(here, here), check_vma=False
    )
```

```python
import functools

import jax
import jax.numpy as jnp
from jax import lax
from jax.experimental import pallas as pl
from jax.experimental.pallas import tpu as pltpu
from jax.sharding import PartitionSpec as P

MESH = pl.DeviceIdType.MESH
HALO = 4
STRIDE = 2 * HALO + 1
LANES = 256
EPSILON = 1e-06
F32, BF16 = jnp.float32, jnp.bfloat16

PIECES = (
    (1, 1, 2, 0, 16),
    (-1, 1, 2, 32, 16),
    (1, -1, 1, 48, 16),
    (-1, -1, 1, 80, 16),
    (0, 1, 2, 16, 16),
    (0, -1, 1, 64, 16),
    (1, 0, 0, 0, 64),
    (-1, 0, 0, 128, 64),
)


def nt(a, b):
    return lax.dot_general(a, b, (((1,), (1,)), ((), ())), preferred_element_type=F32)


def nn(a, b):
    return lax.dot_general(a, b, (((1,), (0,)), ((), ())), preferred_element_type=F32)


def split(x):
    hi = x.astype(BF16)
    return hi, (x - hi.astype(F32)).astype(BF16)


def iota(shape, dim):
    return lax.broadcasted_iota(jnp.int32, shape, dim)


def spread(n):
    steps, d = [], 1
    while d < n - 1:
        steps.append(d)
        d *= 2
    return steps


def kernel(
    ngx, ngy, inc_hbm, kinds_hbm, codes_hbm, ops_hbm, valid_hbm, trans_hbm, tmat_hbm,
    state, sums,
    inc_ref, kinds_ref, pairs, trans_v, tmat_v,
    tmhi, tmlo, tmhi_t, tmlo_t, masks, tt, counts, grouped, mid, side, edge, vhi, vlo,
    one_out, one_in, two_out, two_in,
    load_sem, halo_send, halo_recv, ar_send, ar_recv, spread_sem,
):
    gx, gy = lax.axis_index("gx"), lax.axis_index("gy")
    rows, cols, coeffs = inc_ref.shape
    spheres = rows * cols
    slots = pairs.shape[3]
    count_ops, kinds_n = trans_v.shape[0], tmat_v.shape[0]

    def device(dx, dy):
        return (lax.rem(gx + (dx + ngx), ngx), lax.rem(gy + (dy + ngy), ngy))

    def inside_tests(dx, dy):
        tests = []
        for at, n, d in ((gx, ngx, dx), (gy, ngy, dy)):
            if d > 0:
                tests.append(at < n - d)
            elif d < 0:
                tests.append(at >= -d)
        return tests

    def when(dx, dy):
        return pl.when(functools.reduce(jnp.logical_and, inside_tests(dx, dy)))

    def count_at(at, size, d):
        return (at >= d).astype(jnp.int32) + (at < size - d).astype(jnp.int32)

    def there(dx, dy):
        return (gx + dx, gy + dy)
    barrier = pltpu.get_barrier_semaphore()
    for dx, dy, _, _, _ in PIECES:

        @when(dx, dy)
        def _():
            pl.semaphore_signal(barrier, inc=1, device_id=there(dx, dy), device_id_type=MESH)

    def load(src, dst, n):
        copy = pltpu.make_async_copy(src, dst, load_sem.at[n])
        copy.start()
        return copy

    early = [load(tmat_hbm, tmat_v, 0), load(inc_hbm, inc_ref, 1), load(kinds_hbm, kinds_ref, 2)]

    rounds = [[(0, d) for d in spread(ngy)], [(d, 0) for d in spread(ngx)]]

    def tell(n):
        for axis, steps in enumerate(rounds):
            if n < len(steps):
                dx, dy = steps[n]
                for sign in (1, -1):

                    @when(sign * dx, sign * dy)
                    def _():
                        pl.semaphore_signal(
                            spread_sem.at[n], inc=1, device_id=there(sign * dx, sign * dy), device_id_type=MESH
                        )


    def hear(n):
        expected = 0
        for (at, size), steps in zip(((gy, ngy), (gx, ngx)), rounds):
            if n < len(steps):
                expected = expected + count_at(at, size, sum(steps[n]))
        if n < max(map(len, rounds)):
            pl.semaphore_wait(spread_sem.at[n], expected)
    for copy in early:
        copy.wait()
    for n, src in enumerate((codes_hbm, ops_hbm, valid_hbm)):
        load(src, pairs.at[n], 0)
    late = load(trans_hbm, trans_v, 1)
    lane = iota((spheres, LANES), 1)
    eye = iota((cols, cols), 0) == iota((cols, cols), 1)
    kind_col = jnp.concatenate(
        [
            jnp.sum(
                jnp.where(eye, jnp.broadcast_to(kinds_ref[r : r + 1, :], (cols, cols)), 0).astype(F32),
                axis=1, keepdims=True,
            )
            for r in range(rows)
        ],
        axis=0,
    )

    def source_of(u):
        total = None
        for p in range(kinds_n):
            hi, lo = split(jnp.where(kind_col == p, u, 0.0))
            term = nt(hi, tmhi[p]) + nt(lo, tmhi[p]) + nt(hi, tmlo[p])
            total = term if total is None else total + term
        return total

    def apply_kinds(u):
        hi, lo = split(u)
        both = jnp.concatenate([hi, lo], axis=0)
        wide, fine = None, None
        for p in range(kinds_n):
            chosen = both * masks[p]
            term, more = nn(chosen, tmhi_t[p]), nn(chosen[:spheres], tmlo_t[p])
            wide, fine = (term, more) if wide is None else (wide + term, fine + more)
        return jnp.where(lane < coeffs, wide[:spheres] + wide[spheres:] + fine, 0.0)

    def set_field(h, u):
        mid[h, spheres : 2 * spheres, :] = u
        state[h] = u
        for r in range(rows):
            for e, c in ((0, 0), (1, cols - HALO)):
                edge[h, e, HALO * r : HALO * (r + 1), :] = mid[
                    h, spheres + cols * r + c : spheres + cols * r + c + HALO, :
                ]

    def pieces(h):
        for n, (dx, dy, source, first, count) in enumerate(PIECES):
            if source == 0:
                src, dst = mid.at[h, pl.ds(spheres, spheres)], mid.at[h, pl.ds(first, count)]
            else:
                src, dst = edge.at[h, source - 1], side.at[h, pl.ds(first, count)]
            copy = pltpu.make_async_remote_copy(
                src_ref=src, dst_ref=dst, send_sem=halo_send.at[h], recv_sem=halo_recv.at[h],
                device_id=there(dx, dy), device_id_type=MESH,
            )
            yield dx, dy, copy

    def exchange(h):
        for dx, dy, copy in pieces(h):
            when(dx, dy)(copy.start)

    def all_pieces(sem):
        for x in (1, 2):
            for y in (1, 2):

                @pl.when(jnp.logical_and(near_x == x, near_y == y))
                def _():
                    much = counts.at[0, pl.ds(0, 2 * (spheres * x + 16 * y * (x + 1)))]
                    pltpu.make_async_copy(much, much, sem).wait()

    near_x, near_y = count_at(gx, ngx, 1), count_at(gy, ngy, 1)

    for dx, dy, source, first, count in PIECES:

        @pl.when(jnp.logical_not(functools.reduce(jnp.logical_and, inside_tests(-dx, -dy))))
        def _():
            for h in range(2):
                (mid if source == 0 else side)[h, first : first + count, :] = jnp.zeros((count, LANES), F32)

    for p in range(kinds_n):
        hi, lo = split(tmat_v[p])
        tmhi[p] = hi
        tmlo[p] = lo
    state[0] = jnp.zeros((spheres, LANES), F32)
    state[0, :, :coeffs] = source_of(inc_ref[...].reshape(spheres, coeffs))
    set_field(0, state[0])
    pl.semaphore_wait(barrier, (near_x + 1) * (near_y + 1) - 1)
    exchange(0)
    tell(0)
    pltpu.make_async_copy(pairs, pairs, load_sem.at[0]).wait()
    codes = pairs[0].reshape(spheres, slots)
    sphere = iota((spheres, slots), 0)
    row, col = sphere >> 4, sphere & 15
    step_x = (codes * 57) >> 9
    ext_x = row + step_x
    ext_y = col + codes - STRIDE * step_x
    target = jnp.where(
        ext_y < HALO,
        144 + HALO * ext_x + ext_y,
        jnp.where(ext_y < HALO + cols, cols * step_x + ext_y - HALO, 172 + HALO * ext_x + ext_y),
    )
    at_x = gx * rows + ext_x - HALO
    at_y = gy * cols + ext_y - HALO
    inside = (at_x >= 0) & (at_x < ngx * rows) & (at_y >= 0) & (at_y < ngy * cols)
    inside = inside & (pairs[2].reshape(spheres, slots) == 1)
    key = jnp.where(inside, row * count_ops + pairs[1].reshape(spheres, slots), -1)
    target = jnp.concatenate([target[cols * r : cols * (r + 1)] for r in range(rows)], axis=1)
    key = jnp.concatenate([key[cols * r : cols * (r + 1)] for r in range(rows)], axis=1)
    for c in range(cols):
        left = (iota((rows * count_ops, LANES), 0) == key[c : c + 1, :]).astype(F32).astype(BF16)
        right = (iota((LANES, LANES), 0) == target[c : c + 1, :]).astype(F32).astype(BF16)
        tally = nt(left, right)
        for r in range(rows):
            piece = tally[count_ops * r : count_ops * (r + 1)]
            for half in range(2):
                counts[half, pl.ds(r * cols * count_ops + c, count_ops, stride=cols), :] = piece[
                    :, 128 * half : 128 * (half + 1)
                ]

    late.wait()
    hear(0)
    tell(1)
    unit = (iota((LANES, coeffs), 0) == iota((LANES, coeffs), 1)).astype(F32).astype(BF16)
    for k in range(count_ops):
        tt[k, :, :coeffs] = nt(unit, trans_v[k]).astype(BF16)
    for p in range(kinds_n):
        tmhi_t[p, :, :coeffs] = nt(unit, tmhi[p]).astype(BF16)
        tmlo_t[p, :, :coeffs] = nt(unit, tmlo[p]).astype(BF16)
        mask = jnp.where(jnp.broadcast_to(kind_col, (spheres, LANES)) == p, 1.0, 0.0)
        masks[p] = jnp.concatenate([mask, mask], axis=0).astype(BF16)
    def couple(h):
        all_pieces(halo_recv.at[h])
        if h == 0:
            hear(1)
            tell(2)
        hi, lo = split(mid[h])
        vhi[: 3 * spheres], vlo[: 3 * spheres] = hi, lo
        hi, lo = split(side[h])
        vhi[3 * spheres :], vlo[3 * spheres :] = hi, lo
        tail = jnp.zeros((16, LANES), BF16)
        per_row = cols * count_ops
        for r in range(rows):
            table = jnp.concatenate(
                [counts[half, per_row * r : per_row * (r + 1), :].astype(BF16) for half in range(2)], axis=1
            )
            near = [
                jnp.concatenate([v[cols * r : cols * (r + STRIDE)], v[3 * spheres :], tail], axis=0)
                for v in (vhi, vlo)
            ]
            grouped[per_row * r : per_row * (r + 1), :] = nn(table, near[0]) + nn(table, near[1])
        total = None
        for k in range(count_ops):
            part = jnp.concatenate(
                [grouped[per_row * r + cols * k : per_row * r + cols * (k + 1), :] for r in range(rows)], axis=0
            )
            hi, lo = split(part)
            term = nn(jnp.concatenate([hi, lo], axis=0), tt[k])
            total = term if total is None else total + term
        moved = jnp.where(lane < coeffs, total[:spheres] + total[spheres:], 0.0)
        result = apply_kinds(moved)
        return result

    once = couple(0)
    set_field(1, once)
    exchange(1)
    hear(2)
    tell(3)
    second = couple(1)
    state[2] = second
    base, once = state[0], state[1]

    def inner(a, b):
        return jnp.sum(jnp.sum(a * b, axis=0, keepdims=True), axis=1, keepdims=True)

    products = (
        inner(base, base), inner(base, once), inner(once, once),
        inner(base, second), inner(once, second), inner(second, second),
    )
    slot = iota((1, 128), 1)
    packed = jnp.zeros((1, 128), F32)
    for n, value in enumerate(products):
        packed = jnp.where(slot == n, value, packed)
    def all_sum(n, value, out, into, peers):
        out[...] = value
        for d, peer in enumerate(peers):
            pltpu.make_async_remote_copy(
                src_ref=out, dst_ref=into.at[d], send_sem=ar_send, recv_sem=ar_recv.at[n],
                device_id=peer, device_id_type=MESH,
            ).start()
        pltpu.make_async_copy(into, into, ar_recv.at[n]).wait()
        pltpu.make_async_copy(into, into, ar_send).wait()
        total = value
        for d in range(len(peers)):
            total = total + into[d]
        return total

    def far_first(n, inner):
        def hops(d):
            return min(d // inner, n // inner - d // inner) + min(d % inner, inner - d % inner)

        return sorted(range(1, n), key=lambda d: -hops(d))
    hear(3)
    tell(4)
    packed = all_sum(0, packed, one_out, one_in, [device(d, 0) for d in far_first(ngx, 2)])
    hear(4)
    packed = all_sum(1, packed, two_out, two_in, [device(0, d) for d in far_first(ngy, 8)])
    sums[...] = packed
    all_pieces(halo_send.at[0])
    all_pieces(halo_send.at[1])


def combine(state, sums, sol_ref, res_ref):
    rows, cols, coeffs = sol_ref.shape
    packed = sums[...]
    slot = iota((1, 128), 1)
    base, once, second = [state[n][:, :coeffs] for n in range(3)]

    def entry(n):
        return jnp.sum(jnp.where(slot == n, packed, 0.0), axis=1, keepdims=True)

    g00, g01, g11, g02, g12, g22 = [entry(n) for n in range(6)]
    gram = ((g00, g01, g02), (g01, g11, g12), (g02, g12, g22))

    def pair(a, b):
        total = None
        for i in range(3):
            for j in range(3):
                if a[i] is not None and b[j] is not None:
                    term = a[i] * b[j] * gram[i][j]
                    total = term if total is None else total + term
        return total

    beta2 = g00 + EPSILON
    beta = jnp.sqrt(beta2)
    ib = 1.0 / beta
    shift = (g01 + EPSILON) * ib * ib
    h11 = (g00 - g01) * ib * ib
    rest = (shift * ib, -ib, None)
    h21 = jnp.sqrt(jnp.maximum(pair(rest, rest), 0.0) + EPSILON)
    q = ib / h21
    v1 = (ib, None, None)
    v2 = (shift * q, -q, None)
    m2 = (shift * q, -(1.0 + shift) * q, q)
    h12 = pair(m2, v1)
    left = (m2[0] - h12 * ib, m2[1], m2[2])
    h22 = pair(left, v2)
    left = (left[0] - h22 * v2[0], left[1] - h22 * v2[1], left[2])
    h32 = jnp.sqrt(jnp.maximum(pair(left, left), 0.0) + EPSILON)
    aa = h11 * h11 + h21 * h21
    ab = h11 * h12 + h21 * h22
    bb = h12 * h12 + h22 * h22 + h32 * h32
    ra, rb = beta * h11, beta * h12
    determ = aa * bb - ab * ab
    y1 = (bb * ra - ab * rb) / determ
    y2 = (aa * rb - ab * ra) / determ
    s0 = y1 * ib + y2 * v2[0]
    s1 = y2 * v2[1]
    r0 = 1.0 - s0
    r1 = y1 * ib - y2 * m2[1]
    r2 = -y2 * q
    sol_ref[...] = (s0 * base + s1 * once).reshape(rows, cols, coeffs)
    res_ref[...] = (r0 * base + r1 * once + r2 * second).reshape(rows, cols, coeffs)


def solution(mesh):
    ngx, ngy = mesh.shape["gx"], mesh.shape["gy"]

    def body(incident, sphere_kinds, pair_codes, operators, pair_valid, translations, tmatrices):
        rows, cols, coeffs = incident.shape
        spheres = rows * cols
        count_ops, kinds_n = translations.shape[0], tmatrices.shape[0]
        vmem = pl.BlockSpec(memory_space=pltpu.VMEM)
        hbm = pl.BlockSpec(memory_space=pltpu.HBM)
        args = (incident, sphere_kinds, pair_codes, operators, pair_valid, translations, tmatrices)
        held = [(arg.shape, arg.dtype) for arg in args]
        held[2:5] = [((3, *pair_codes.shape), jnp.int32)]
        state, sums = pl.pallas_call(
            functools.partial(kernel, ngx, ngy),
            out_shape=(pltpu.VMEM((3, spheres, LANES), F32), pltpu.VMEM((1, 128), F32)),
            in_specs=[hbm] * 7,
            out_specs=(vmem, vmem),
            scratch_shapes=[pltpu.VMEM(shape, kind) for shape, kind in held]
            + [pltpu.VMEM(tmatrices.shape, BF16)] * 2
            + [pltpu.VMEM((kinds_n, LANES, LANES), BF16)] * 2
            + [
                pltpu.VMEM((kinds_n, 2 * spheres, LANES), BF16),
                pltpu.VMEM((count_ops, LANES, LANES), BF16),
                pltpu.VMEM((2, spheres * count_ops, 128), F32),
                pltpu.VMEM((spheres * count_ops, LANES), F32),
                pltpu.VMEM((2, 3 * spheres, LANES), F32),
                pltpu.VMEM((2, 96, LANES), F32),
                pltpu.VMEM((2, 2, 16, LANES), F32),
                pltpu.VMEM((3 * spheres + 96, LANES), BF16),
                pltpu.VMEM((3 * spheres + 96, LANES), BF16),
                pltpu.VMEM((1, 128), F32),
                pltpu.VMEM((ngx - 1, 1, 128), F32),
                pltpu.VMEM((1, 128), F32),
                pltpu.VMEM((ngy - 1, 1, 128), F32),
                pltpu.SemaphoreType.DMA((3,)),
                pltpu.SemaphoreType.DMA((2,)),
                pltpu.SemaphoreType.DMA((2,)),
                pltpu.SemaphoreType.DMA,
                pltpu.SemaphoreType.DMA((2,)),
                pltpu.SemaphoreType.REGULAR((5,)),
            ],
            compiler_params=pltpu.CompilerParams(collective_id=0, has_side_effects=True),
        )(*args)
        state, sums = [pltpu.with_memory_space_constraint(x, pltpu.VMEM) for x in (state, sums)]
        return pl.pallas_call(
            combine,
            out_shape=(jax.ShapeDtypeStruct(incident.shape, F32),) * 2,
            in_specs=[vmem] * 2,
            out_specs=(vmem, vmem),
        )(state, sums)

    here, line, table = P("gx", "gy", None), P("gx", "gy"), P()
    return jax.shard_map(
        body, mesh=mesh, in_specs=(here, line, here, here, here, table, table), out_specs=(here, here), check_vma=False
    )
```

```python
import functools

import jax
import jax.numpy as jnp
from jax import lax
from jax.experimental import pallas as pl
from jax.experimental.pallas import tpu as pltpu
from jax.sharding import PartitionSpec as P

MESH = pl.DeviceIdType.MESH
HALO = 4
STRIDE = 2 * HALO + 1
LANES = 256
EPSILON = 1e-06
F32, BF16 = jnp.float32, jnp.bfloat16

PIECES = (
    (1, 1, 2, 0, 16),
    (-1, 1, 2, 32, 16),
    (1, -1, 1, 48, 16),
    (-1, -1, 1, 80, 16),
    (0, 1, 2, 16, 16),
    (0, -1, 1, 64, 16),
    (1, 0, 0, 0, 64),
    (-1, 0, 0, 128, 64),
)


def nt(a, b):
    return lax.dot_general(a, b, (((1,), (1,)), ((), ())), preferred_element_type=F32)


def nn(a, b):
    return lax.dot_general(a, b, (((1,), (0,)), ((), ())), preferred_element_type=F32)


def split(x):
    hi = x.astype(BF16)
    return hi, (x - hi.astype(F32)).astype(BF16)


def iota(shape, dim):
    return lax.broadcasted_iota(jnp.int32, shape, dim)


def spread(n):
    steps, d = [], 1
    while d < n - 1:
        steps.append(d)
        d *= 2
    return steps


def kernel(
    ngx, ngy, inc_hbm, kinds_hbm, codes_hbm, ops_hbm, valid_hbm, trans_hbm, tmat_hbm,
    state, sums,
    inc_ref, kinds_ref, pairs, trans_v, tmat_v,
    tmhi, tmlo, tmhi_t, tmlo_t, masks, tt, counts, grouped, mid, side, edge, vhi, vlo,
    one_out, one_in, two_out, two_in,
    load_sem, halo_send, halo_recv, ar_send, ar_recv, spread_sem,
):
    gx, gy = lax.axis_index("gx"), lax.axis_index("gy")
    rows, cols, coeffs = inc_ref.shape
    spheres = rows * cols
    slots = pairs.shape[3]
    count_ops, kinds_n = trans_v.shape[0], tmat_v.shape[0]

    def device(dx, dy):
        return (lax.rem(gx + (dx + ngx), ngx), lax.rem(gy + (dy + ngy), ngy))

    def inside_tests(dx, dy):
        tests = []
        for at, n, d in ((gx, ngx, dx), (gy, ngy, dy)):
            if d > 0:
                tests.append(at < n - d)
            elif d < 0:
                tests.append(at >= -d)
        return tests

    def when(dx, dy):
        return pl.when(functools.reduce(jnp.logical_and, inside_tests(dx, dy)))

    def count_at(at, size, d):
        return (at >= d).astype(jnp.int32) + (at < size - d).astype(jnp.int32)

    def there(dx, dy):
        return (gx + dx, gy + dy)
    barrier = pltpu.get_barrier_semaphore()
    for dx, dy, _, _, _ in PIECES:

        @when(dx, dy)
        def _():
            pl.semaphore_signal(barrier, inc=1, device_id=there(dx, dy), device_id_type=MESH)

    def load(src, dst, n):
        copy = pltpu.make_async_copy(src, dst, load_sem.at[n])
        copy.start()
        return copy

    early = [load(tmat_hbm, tmat_v, 0), load(inc_hbm, inc_ref, 1), load(kinds_hbm, kinds_ref, 2)]

    rounds = [[(0, d) for d in spread(ngy)], [(d, 0) for d in spread(ngx)]]

    def tell(n):
        for axis, steps in enumerate(rounds):
            if n < len(steps):
                dx, dy = steps[n]
                for sign in (1, -1):

                    @when(sign * dx, sign * dy)
                    def _():
                        pl.semaphore_signal(
                            spread_sem.at[n], inc=1, device_id=there(sign * dx, sign * dy), device_id_type=MESH
                        )


    def hear(n):
        expected = 0
        for (at, size), steps in zip(((gy, ngy), (gx, ngx)), rounds):
            if n < len(steps):
                expected = expected + count_at(at, size, sum(steps[n]))
        if n < max(map(len, rounds)):
            pl.semaphore_wait(spread_sem.at[n], expected)
    for copy in early:
        copy.wait()
    for n, src in enumerate((codes_hbm, ops_hbm, valid_hbm)):
        load(src, pairs.at[n], 0)
    late = load(trans_hbm, trans_v, 1)
    lane = iota((spheres, LANES), 1)
    eye = iota((cols, cols), 0) == iota((cols, cols), 1)
    kind_col = jnp.concatenate(
        [
            jnp.sum(
                jnp.where(eye, jnp.broadcast_to(kinds_ref[r : r + 1, :], (cols, cols)), 0).astype(F32),
                axis=1, keepdims=True,
            )
            for r in range(rows)
        ],
        axis=0,
    )

    def source_of(u):
        total = None
        for p in range(kinds_n):
            hi, lo = split(jnp.where(kind_col == p, u, 0.0))
            term = nt(hi, tmhi[p]) + nt(lo, tmhi[p]) + nt(hi, tmlo[p])
            total = term if total is None else total + term
        return total

    def apply_kinds(u):
        hi, lo = split(u)
        both = jnp.concatenate([hi, lo], axis=0)
        wide, fine = None, None
        for p in range(kinds_n):
            chosen = both * masks[p]
            term, more = nn(chosen, tmhi_t[p]), nn(chosen[:spheres], tmlo_t[p])
            wide, fine = (term, more) if wide is None else (wide + term, fine + more)
        return jnp.where(lane < coeffs, wide[:spheres] + wide[spheres:] + fine, 0.0)

    def set_field(h, u):
        mid[h, spheres : 2 * spheres, :] = u
        state[h] = u
        for r in range(rows):
            for e, c in ((0, 0), (1, cols - HALO)):
                edge[h, e, HALO * r : HALO * (r + 1), :] = mid[
                    h, spheres + cols * r + c : spheres + cols * r + c + HALO, :
                ]

    def pieces(h):
        for n, (dx, dy, source, first, count) in enumerate(PIECES):
            if source == 0:
                src, dst = mid.at[h, pl.ds(spheres, spheres)], mid.at[h, pl.ds(first, count)]
            else:
                src, dst = edge.at[h, source - 1], side.at[h, pl.ds(first, count)]
            copy = pltpu.make_async_remote_copy(
                src_ref=src, dst_ref=dst, send_sem=halo_send.at[h], recv_sem=halo_recv.at[h],
                device_id=there(dx, dy), device_id_type=MESH,
            )
            yield dx, dy, copy

    def exchange(h):
        for dx, dy, copy in pieces(h):
            when(dx, dy)(copy.start)

    def all_pieces(sem):
        for x in (1, 2):
            for y in (1, 2):

                @pl.when(jnp.logical_and(near_x == x, near_y == y))
                def _():
                    much = counts.at[0, pl.ds(0, 2 * (spheres * x + 16 * y * (x + 1)))]
                    pltpu.make_async_copy(much, much, sem).wait()

    near_x, near_y = count_at(gx, ngx, 1), count_at(gy, ngy, 1)

    for dx, dy, source, first, count in PIECES:

        @pl.when(jnp.logical_not(functools.reduce(jnp.logical_and, inside_tests(-dx, -dy))))
        def _():
            for h in range(2):
                (mid if source == 0 else side)[h, first : first + count, :] = jnp.zeros((count, LANES), F32)

    for p in range(kinds_n):
        hi, lo = split(tmat_v[p])
        tmhi[p] = hi
        tmlo[p] = lo
    state[0] = jnp.zeros((spheres, LANES), F32)
    state[0, :, :coeffs] = source_of(inc_ref[...].reshape(spheres, coeffs))
    set_field(0, state[0])
    pl.semaphore_wait(barrier, (near_x + 1) * (near_y + 1) - 1)
    exchange(0)
    tell(0)
    pltpu.make_async_copy(pairs, pairs, load_sem.at[0]).wait()
    codes = pairs[0].reshape(spheres, slots)
    sphere = iota((spheres, slots), 0)
    row, col = sphere >> 4, sphere & 15
    step_x = (codes * 57) >> 9
    ext_x = row + step_x
    ext_y = col + codes - STRIDE * step_x
    target = jnp.where(
        ext_y < HALO,
        144 + HALO * ext_x + ext_y,
        jnp.where(ext_y < HALO + cols, cols * step_x + ext_y - HALO, 172 + HALO * ext_x + ext_y),
    )
    at_x = gx * rows + ext_x - HALO
    at_y = gy * cols + ext_y - HALO
    inside = (at_x >= 0) & (at_x < ngx * rows) & (at_y >= 0) & (at_y < ngy * cols)
    inside = inside & (pairs[2].reshape(spheres, slots) == 1)
    key = jnp.where(inside, row * count_ops + pairs[1].reshape(spheres, slots), -1)
    target = jnp.concatenate([target[cols * r : cols * (r + 1)] for r in range(rows)], axis=1)
    key = jnp.concatenate([key[cols * r : cols * (r + 1)] for r in range(rows)], axis=1)
    for c in range(cols):
        left = (iota((rows * count_ops, LANES), 0) == key[c : c + 1, :]).astype(F32).astype(BF16)
        right = (iota((LANES, LANES), 0) == target[c : c + 1, :]).astype(F32).astype(BF16)
        tally = nt(left, right)
        for r in range(rows):
            piece = tally[count_ops * r : count_ops * (r + 1)]
            for half in range(2):
                counts[half, pl.ds(r * cols * count_ops + c, count_ops, stride=cols), :] = piece[
                    :, 128 * half : 128 * (half + 1)
                ]

    late.wait()
    hear(0)
    tell(1)
    unit = (iota((LANES, coeffs), 0) == iota((LANES, coeffs), 1)).astype(F32).astype(BF16)
    for k in range(count_ops):
        tt[k, :, :coeffs] = nt(unit, trans_v[k]).astype(BF16)
    for p in range(kinds_n):
        tmhi_t[p, :, :coeffs] = nt(unit, tmhi[p]).astype(BF16)
        tmlo_t[p, :, :coeffs] = nt(unit, tmlo[p]).astype(BF16)
        mask = jnp.where(jnp.broadcast_to(kind_col, (spheres, LANES)) == p, 1.0, 0.0)
        masks[p] = jnp.concatenate([mask, mask], axis=0).astype(BF16)
    def couple(h):
        all_pieces(halo_recv.at[h])
        hi, lo = split(mid[h])
        vhi[: 3 * spheres], vlo[: 3 * spheres] = hi, lo
        hi, lo = split(side[h])
        vhi[3 * spheres :], vlo[3 * spheres :] = hi, lo
        tail = jnp.zeros((16, LANES), BF16)
        per_row = cols * count_ops
        for r in range(rows):
            table = jnp.concatenate(
                [counts[half, per_row * r : per_row * (r + 1), :].astype(BF16) for half in range(2)], axis=1
            )
            near = [
                jnp.concatenate([v[cols * r : cols * (r + STRIDE)], v[3 * spheres :], tail], axis=0)
                for v in (vhi, vlo)
            ]
            grouped[per_row * r : per_row * (r + 1), :] = nn(table, near[0]) + nn(table, near[1])
        total = None
        for k in range(count_ops):
            part = jnp.concatenate(
                [grouped[per_row * r + cols * k : per_row * r + cols * (k + 1), :] for r in range(rows)], axis=0
            )
            hi, lo = split(part)
            term = nn(jnp.concatenate([hi, lo], axis=0), tt[k])
            total = term if total is None else total + term
        moved = jnp.where(lane < coeffs, total[:spheres] + total[spheres:], 0.0)
        if h == 0:
            hear(1)
            tell(2)
        result = apply_kinds(moved)
        return result

    once = couple(0)
    set_field(1, once)
    exchange(1)
    hear(2)
    tell(3)
    second = couple(1)
    state[2] = second
    base, once = state[0], state[1]

    def inner(a, b):
        return jnp.sum(jnp.sum(a * b, axis=0, keepdims=True), axis=1, keepdims=True)

    products = (
        inner(base, base), inner(base, once), inner(once, once),
        inner(base, second), inner(once, second), inner(second, second),
    )
    slot = iota((1, 128), 1)
    packed = jnp.zeros((1, 128), F32)
    for n, value in enumerate(products):
        packed = jnp.where(slot == n, value, packed)
    def all_sum(n, value, out, into, peers):
        out[...] = value
        for d, peer in enumerate(peers):
            pltpu.make_async_remote_copy(
                src_ref=out, dst_ref=into.at[d], send_sem=ar_send, recv_sem=ar_recv.at[n],
                device_id=peer, device_id_type=MESH,
            ).start()
        pltpu.make_async_copy(into, into, ar_recv.at[n]).wait()
        pltpu.make_async_copy(into, into, ar_send).wait()
        total = value
        for d in range(len(peers)):
            total = total + into[d]
        return total

    def far_first(n, inner):
        def hops(d):
            return min(d // inner, n // inner - d // inner) + min(d % inner, inner - d % inner)

        return sorted(range(1, n), key=lambda d: -hops(d))
    hear(3)
    tell(4)
    packed = all_sum(0, packed, one_out, one_in, [device(d, 0) for d in far_first(ngx, 2)])
    hear(4)
    packed = all_sum(1, packed, two_out, two_in, [device(0, d) for d in far_first(ngy, 8)])
    sums[...] = packed
    all_pieces(halo_send.at[0])
    all_pieces(halo_send.at[1])


def combine(state, sums, sol_ref, res_ref):
    rows, cols, coeffs = sol_ref.shape
    packed = sums[...]
    slot = iota((1, 128), 1)
    base, once, second = [state[n][:, :coeffs] for n in range(3)]

    def entry(n):
        return jnp.sum(jnp.where(slot == n, packed, 0.0), axis=1, keepdims=True)

    g00, g01, g11, g02, g12, g22 = [entry(n) for n in range(6)]
    gram = ((g00, g01, g02), (g01, g11, g12), (g02, g12, g22))

    def pair(a, b):
        total = None
        for i in range(3):
            for j in range(3):
                if a[i] is not None and b[j] is not None:
                    term = a[i] * b[j] * gram[i][j]
                    total = term if total is None else total + term
        return total

    beta2 = g00 + EPSILON
    beta = jnp.sqrt(beta2)
    ib = 1.0 / beta
    shift = (g01 + EPSILON) * ib * ib
    h11 = (g00 - g01) * ib * ib
    rest = (shift * ib, -ib, None)
    h21 = jnp.sqrt(jnp.maximum(pair(rest, rest), 0.0) + EPSILON)
    q = ib / h21
    v1 = (ib, None, None)
    v2 = (shift * q, -q, None)
    m2 = (shift * q, -(1.0 + shift) * q, q)
    h12 = pair(m2, v1)
    left = (m2[0] - h12 * ib, m2[1], m2[2])
    h22 = pair(left, v2)
    left = (left[0] - h22 * v2[0], left[1] - h22 * v2[1], left[2])
    h32 = jnp.sqrt(jnp.maximum(pair(left, left), 0.0) + EPSILON)
    aa = h11 * h11 + h21 * h21
    ab = h11 * h12 + h21 * h22
    bb = h12 * h12 + h22 * h22 + h32 * h32
    ra, rb = beta * h11, beta * h12
    determ = aa * bb - ab * ab
    y1 = (bb * ra - ab * rb) / determ
    y2 = (aa * rb - ab * ra) / determ
    s0 = y1 * ib + y2 * v2[0]
    s1 = y2 * v2[1]
    r0 = 1.0 - s0
    r1 = y1 * ib - y2 * m2[1]
    r2 = -y2 * q
    sol_ref[...] = (s0 * base + s1 * once).reshape(rows, cols, coeffs)
    res_ref[...] = (r0 * base + r1 * once + r2 * second).reshape(rows, cols, coeffs)


def solution(mesh):
    ngx, ngy = mesh.shape["gx"], mesh.shape["gy"]

    def body(incident, sphere_kinds, pair_codes, operators, pair_valid, translations, tmatrices):
        rows, cols, coeffs = incident.shape
        spheres = rows * cols
        count_ops, kinds_n = translations.shape[0], tmatrices.shape[0]
        vmem = pl.BlockSpec(memory_space=pltpu.VMEM)
        hbm = pl.BlockSpec(memory_space=pltpu.HBM)
        args = (incident, sphere_kinds, pair_codes, operators, pair_valid, translations, tmatrices)
        held = [(arg.shape, arg.dtype) for arg in args]
        held[2:5] = [((3, *pair_codes.shape), jnp.int32)]
        state, sums = pl.pallas_call(
            functools.partial(kernel, ngx, ngy),
            out_shape=(pltpu.VMEM((3, spheres, LANES), F32), pltpu.VMEM((1, 128), F32)),
            in_specs=[hbm] * 7,
            out_specs=(vmem, vmem),
            scratch_shapes=[pltpu.VMEM(shape, kind) for shape, kind in held]
            + [pltpu.VMEM(tmatrices.shape, BF16)] * 2
            + [pltpu.VMEM((kinds_n, LANES, LANES), BF16)] * 2
            + [
                pltpu.VMEM((kinds_n, 2 * spheres, LANES), BF16),
                pltpu.VMEM((count_ops, LANES, LANES), BF16),
                pltpu.VMEM((2, spheres * count_ops, 128), F32),
                pltpu.VMEM((spheres * count_ops, LANES), F32),
                pltpu.VMEM((2, 3 * spheres, LANES), F32),
                pltpu.VMEM((2, 96, LANES), F32),
                pltpu.VMEM((2, 2, 16, LANES), F32),
                pltpu.VMEM((3 * spheres + 96, LANES), BF16),
                pltpu.VMEM((3 * spheres + 96, LANES), BF16),
                pltpu.VMEM((1, 128), F32),
                pltpu.VMEM((ngx - 1, 1, 128), F32),
                pltpu.VMEM((1, 128), F32),
                pltpu.VMEM((ngy - 1, 1, 128), F32),
                pltpu.SemaphoreType.DMA((3,)),
                pltpu.SemaphoreType.DMA((2,)),
                pltpu.SemaphoreType.DMA((2,)),
                pltpu.SemaphoreType.DMA,
                pltpu.SemaphoreType.DMA((2,)),
                pltpu.SemaphoreType.REGULAR((5,)),
            ],
            compiler_params=pltpu.CompilerParams(collective_id=0, has_side_effects=True),
        )(*args)
        state, sums = [pltpu.with_memory_space_constraint(x, pltpu.VMEM) for x in (state, sums)]
        return pl.pallas_call(
            combine,
            out_shape=(jax.ShapeDtypeStruct(incident.shape, F32),) * 2,
            in_specs=[vmem] * 2,
            out_specs=(vmem, vmem),
        )(state, sums)

    here, line, table = P("gx", "gy", None), P("gx", "gy"), P()
    return jax.shard_map(
        body, mesh=mesh, in_specs=(here, line, here, here, here, table, table), out_specs=(here, here), check_vma=False
    )
```
